512 devices in a mesh: grp: 4 (over x), chan: 128 (over y, z, core).
Axes of the slice: x: 4, y: 4, z: 16, core: 2. Of those that a mesh axis runs over, the one named last changes fastest.
Arguments:
- visibilities: float32 [4, 2, 128, 16, 2, 2048], P('grp', None, 'chan'), may hold values from -12 to 12
- model: bfloat16 [4, 2, 8, 128, 16, 2, 2048], P('grp', None, None, 'chan'), may hold values from -6 to 6
- flags: int32 [4, 128, 16, 2, 2048], P('grp', 'chan'), may hold values 0 or 1
- antennas: int32 [4, 2, 2048], P('grp'), may hold values from 0 to 63, as said below
- correlation: int32 [4, 4, 40], replicated, may hold values from -1 to 63, as said below
- gains_init: float32 [4, 2, 8, 128, 16, 64], P('grp', None, None, 'chan'), may hold values from -4 to 4
Outputs:
- final_jones_matrices: float32 [4, 2, 8, 128, 16, 64], P('grp', None, None, 'chan')
- consensus: float32 [4, 2, 8, 128, 16, 64], P('grp', None, None, 'chan')
- residual_vis: float32 [4, 2, 128, 16, 2, 2048], P('grp', None, 'chan')
The draws below stay inside these ranges and needn't reach their ends.
Inputs may be any that keep to these rules, and one draw needn't show every extreme that they name: antennas[g, 0, b] and antennas[g, 1, b] are different slots. correlation[g, h, j] and correlation[h, g, j] are the slots in clusters g and h of one shared station, or both -1; the live entries of a list are a prefix of it and distinct; correlation[g, g] is all -1; each pair of clusters shares 40 // 2 to 40 stations, and some pair exactly 40.
All inputs are finite; a program needn't handle non-finite values. No bound on the sum of `flags` on one device may be relied on, other than what follows from the above.
Results may differ from the reference program's by a relative error of at most 0.0003.
Values sent between devices are 32-bit elements; how exact they have to be, the bound alone decides.
No kernel may reach another device: no remote copies, remote signals or barrier semaphores. Data moves between devices by JAX's collectives and lax.ppermute only.
A program may use at most 64 MiB of HBM per device.

```python
import jax
import jax.numpy as jnp
from jax import lax

K = 8
ST = 64
SHARED = 40
BL = 2048
SI = 16
TS = 2
ITERS = 2
CLUSTERS = 4
CHANNELS = 128


def draw_antennas(key, part):
    key_one, key_two = jax.random.split(jax.random.fold_in(key, 11))
    first = jax.random.randint(key_one, (CLUSTERS, BL), 0, ST)
    offset = jax.random.randint(key_two, (CLUSTERS, BL), 1, ST)
    second = (first + offset) % ST
    return jnp.stack([first, second], axis=1).astype(jnp.int32)


def draw_correlation(key, part):
    table = -jnp.ones((CLUSTERS, CLUSTERS, SHARED), jnp.int32)
    for cluster_index in range(CLUSTERS):
        for other in range(cluster_index + 1, CLUSTERS):
            subkey = jax.random.fold_in(key, 100 + cluster_index * CLUSTERS + other)
            key_one, key_two, key_three = jax.random.split(subkey, 3)
            live = jax.random.randint(key_three, (), SHARED // 2, SHARED + 1)
            if cluster_index == 0 and other == 1:
                live = jnp.int32(SHARED)
            keep = jnp.arange(SHARED, dtype=jnp.int32) < live
            slots_mine = jax.random.permutation(key_one, ST)[:SHARED].astype(jnp.int32)
            slots_theirs = jax.random.permutation(key_two, ST)[:SHARED].astype(jnp.int32)
            table = table.at[cluster_index, other].set(jnp.where(keep, slots_mine, -1))
            table = table.at[other, cluster_index].set(jnp.where(keep, slots_theirs, -1))
    return table


def set_ends(array, stream_key, least, largest):
    spot = [jax.random.randint(jax.random.fold_in(stream_key, axis), (), 0, length) for axis, length in enumerate(array.shape)]
    widest = array.shape.index(max(array.shape))
    beside = spot[:widest] + [(spot[widest] + 1) % array.shape[widest]] + spot[widest + 1:]
    return array.at[tuple(spot)].set(least).at[tuple(beside)].set(largest)


def block_levels(stream_key, extent, pieces, smallest, largest):
    gain = 1.0
    for dim, shards_of in pieces:
        steps = jax.random.uniform(jax.random.fold_in(jax.random.fold_in(stream_key, 6), dim), (shards_of,), jnp.float32, smallest / len(pieces), largest / len(pieces))
        gain = gain * jnp.repeat(jnp.exp(steps), extent[dim] // shards_of).reshape((-1,) + (1,) * (len(extent) - 1 - dim))
    return gain


def centred(stream_key, dims, width, most, pieces=(), held_as=jnp.bfloat16):
    loudness = block_levels(stream_key, dims, pieces, -0.22, 0.18) if pieces else 1.0
    array = jax.random.normal(stream_key, dims, jnp.float32) * width * loudness
    return jnp.minimum(jnp.maximum(array, -most), most).astype(held_as)


def setup_inputs(seed: int = 0) -> dict:
    splits = jax.random.split(jax.random.key(seed), 7)
    return {
        "visibilities": centred(splits[0], (CLUSTERS, 2, CHANNELS, SI, TS, BL), 2.0, 12.0, ((0, 4), (2, 128)), jnp.float32),
        "model": centred(splits[1], (CLUSTERS, 2, K, CHANNELS, SI, TS, BL), 1.0, 6.0, ((0, 4), (3, 128))),
        "flags": set_ends((jax.random.randint(splits[2], (CLUSTERS, CHANNELS, SI, TS, BL), 0, 8) < 1).astype(jnp.int32), jax.random.fold_in(splits[2], 1), 0, 1),
        "antennas": draw_antennas(jax.random.fold_in(splits[6], 71), 0),
        "correlation": draw_correlation(jax.random.fold_in(splits[6], 71), 0),
        "gains_init": centred(splits[5], (CLUSTERS, 2, K, CHANNELS, SI, ST), 0.8, 4.0, ((0, 4), (3, 128)), jnp.float32),
    }


def poly_basis(count):
    freq = jnp.arange(count, dtype=jnp.float32)
    xval = (2.0 * freq + 1.0) / count - 1.0
    return jnp.stack([jnp.ones_like(xval), xval, 1.5 * xval * xval - 0.5], axis=1)


def gram_inverse(basis):
    gram = jnp.dot(basis.T, basis, precision=lax.Precision.HIGHEST)
    cross_one = jnp.cross(gram[1], gram[2])
    cross_two = jnp.cross(gram[2], gram[0])
    cross_three = jnp.cross(gram[0], gram[1])
    determinant = jnp.sum(gram[0] * cross_one)
    return jnp.stack([cross_one, cross_two, cross_three], axis=1) / determinant


def model_terms(leading_receiver_jones, trailing_receiver_jones, vis, model, flag):
    model_re = model[0].astype(jnp.float32)
    model_im = model[1].astype(jnp.float32)
    weight = (1 - flag).astype(jnp.float32)
    prod_re = leading_receiver_jones[0] * trailing_receiver_jones[0] + leading_receiver_jones[1] * trailing_receiver_jones[1]
    prod_im = leading_receiver_jones[1] * trailing_receiver_jones[0] - leading_receiver_jones[0] * trailing_receiver_jones[1]
    pred_re = prod_re * model_re - prod_im * model_im
    pred_im = prod_re * model_im + prod_im * model_re
    res_re = weight * (vis[0] - jnp.sum(pred_re, axis=0))
    res_im = weight * (vis[1] - jnp.sum(pred_im, axis=0))
    return model_re, model_im, weight, pred_re, pred_im, res_re, res_im


def station_sides(leading_receiver_jones, trailing_receiver_jones, terms):
    model_re, model_im, weight, pred_re, pred_im, res_re, res_im = terms
    resid_re = res_re + weight * pred_re
    resid_im = res_im + weight * pred_im
    zed_re = trailing_receiver_jones[0] * model_re + trailing_receiver_jones[1] * model_im
    zed_im = trailing_receiver_jones[0] * model_im - trailing_receiver_jones[1] * model_re
    ups_re = leading_receiver_jones[0] * model_re - leading_receiver_jones[1] * model_im
    ups_im = leading_receiver_jones[0] * model_im + leading_receiver_jones[1] * model_re
    first_station_side = jnp.stack([
        jnp.sum(resid_re * zed_re + resid_im * zed_im, axis=-2),
        jnp.sum(resid_im * zed_re - resid_re * zed_im, axis=-2),
        jnp.sum(weight * (zed_re * zed_re + zed_im * zed_im), axis=-2)])
    second_station_side = jnp.stack([
        jnp.sum(resid_re * ups_re + resid_im * ups_im, axis=-2),
        jnp.sum(resid_re * ups_im - resid_im * ups_re, axis=-2),
        jnp.sum(weight * (ups_re * ups_re + ups_im * ups_im), axis=-2)])
    return first_station_side, second_station_side


def new_gains(summed_totals, target, penalty):
    return jnp.stack([(summed_totals[0] + penalty * target[0]) / (summed_totals[2] + penalty),
                      (summed_totals[1] + penalty * target[1]) / (summed_totals[2] + penalty)])


def reference(visibilities, model, flags, antennas, correlation, gains_init):
    high = lax.Precision.HIGHEST
    penalty = 2.0 * BL * TS / ST
    basis = poly_basis(CHANNELS)
    ginv = gram_inverse(basis)

    def fitted(values):
        partial_value = jnp.einsum('fn,akfsq->naksq', basis, values, precision=high)
        coef = jnp.einsum('mn,naksq->maksq', ginv, partial_value, precision=high)
        return jnp.einsum('fn,naksq->akfsq', basis, coef, precision=high)

    def segment_ids(side, index):
        moved = jnp.moveaxis(side, -1, 0)
        summed = jax.ops.segment_sum(moved, index, num_segments=ST)
        return jnp.moveaxis(summed, 0, -1)

    def update(cluster_index, final_jones_matrices, target):
        antenna_list = antennas[cluster_index]

        def one_channel(items):
            vis_c, model_c, flag_c, conjugate_gains, target_c = items
            leading_receiver_jones = conjugate_gains[:, :, :, antenna_list[0]][:, :, :, None, :]
            trailing_receiver_jones = conjugate_gains[:, :, :, antenna_list[1]][:, :, :, None, :]
            terms = model_terms(leading_receiver_jones, trailing_receiver_jones, vis_c, model_c, flag_c)
            first_station_side, second_station_side = station_sides(leading_receiver_jones, trailing_receiver_jones, terms)
            summed_totals = segment_ids(first_station_side, antenna_list[0]) + segment_ids(second_station_side, antenna_list[1])
            return new_gains(summed_totals, target_c, penalty)

        items = (jnp.moveaxis(visibilities[cluster_index], 1, 0), jnp.moveaxis(model[cluster_index], 2, 0),
                 flags[cluster_index], jnp.moveaxis(final_jones_matrices, 2, 0), jnp.moveaxis(target, 2, 0))
        return jnp.moveaxis(lax.map(one_channel, items), 0, 2)

    def residual(cluster_index, final_jones_matrices):
        antenna_list = antennas[cluster_index]

        def one_channel(items):
            vis_c, model_c, flag_c, conjugate_gains = items
            leading_receiver_jones = conjugate_gains[:, :, :, antenna_list[0]][:, :, :, None, :]
            trailing_receiver_jones = conjugate_gains[:, :, :, antenna_list[1]][:, :, :, None, :]
            terms = model_terms(leading_receiver_jones, trailing_receiver_jones, vis_c, model_c, flag_c)
            return jnp.stack([terms[5], terms[6]])

        items = (jnp.moveaxis(visibilities[cluster_index], 1, 0), jnp.moveaxis(model[cluster_index], 2, 0),
                 flags[cluster_index], jnp.moveaxis(final_jones_matrices, 2, 0))
        return jnp.moveaxis(lax.map(one_channel, items), 0, 1)

    def average(gains_all):
        shape = gains_all.shape
        flat = gains_all.reshape(CLUSTERS, -1, ST)
        iota = jnp.arange(ST, dtype=jnp.int32)
        result = []
        for cluster_index in range(CLUSTERS):
            total = flat[cluster_index]
            count = jnp.zeros((ST,), jnp.float32)
            for other in range(CLUSTERS):
                sel_mine = (correlation[cluster_index, other][:, None] == iota[None, :]).astype(jnp.float32)
                sel_theirs = (correlation[other, cluster_index][:, None] == iota[None, :]).astype(jnp.float32)
                received = jnp.einsum('js,rs->jr', sel_theirs, flat[other], precision=high)
                total = total + jnp.einsum('js,jr->rs', sel_mine, received, precision=high)
                count = count + jnp.sum(sel_mine, axis=0)
            result.append(total / (1.0 + count))
        return jnp.stack(result).reshape(shape)

    present_jones_matrices = gains_init
    dual = jnp.zeros_like(gains_init)
    agreed = jnp.stack([fitted(present_jones_matrices[c]) for c in range(CLUSTERS)])
    for step in range(ITERS):
        target = agreed - dual
        present_jones_matrices = jnp.stack([update(c, present_jones_matrices[c], target[c]) for c in range(CLUSTERS)])
        present_jones_matrices = average(present_jones_matrices)
        agreed = jnp.stack([fitted(present_jones_matrices[c] + dual[c]) for c in range(CLUSTERS)])
        dual = dual + present_jones_matrices - agreed
    residual_vis = jnp.stack([residual(c, present_jones_matrices[c]) for c in range(CLUSTERS)])
    return present_jones_matrices, agreed, residual_vis
```

```python
import functools

import jax
import jax.numpy as jnp
import numpy as np
from jax import lax
from jax.experimental import pallas as pl
from jax.experimental.pallas import tpu as pltpu
from jax.sharding import PartitionSpec as P

K, SI, ST, BL, CL, CH = 8, 16, 64, 2048, 4, 128
RHO = 128.0
F32, BF16 = jnp.float32, jnp.bfloat16
NT = (((1,), (1,)), ((), ()))
HIGH = lax.Precision.HIGHEST
BC = 256
VM = pl.BlockSpec(memory_space=pltpu.VMEM)
SD = jax.ShapeDtypeStruct


def projector():
    f = np.arange(CH, dtype=np.float64)
    x = (2 * f + 1) / CH - 1
    basis = np.stack([np.ones_like(x), x, 1.5 * x * x - 0.5], axis=1)
    return (basis @ np.linalg.inv(basis.T @ basis) @ basis.T).astype(np.float32)


def split3(x):
    hi=x.astype(BF16); r=x-hi.astype(F32); mid=r.astype(BF16); lo=(r-mid.astype(F32)).astype(BF16)
    return hi,mid,lo

def split2(x):
    hi=x.astype(BF16)
    return hi,(x-hi.astype(F32)).astype(BF16)

def onehot(ants, side, off):
    ids=ants[side:side+1, pl.ds(off,BC)]
    io=lax.broadcasted_iota(jnp.int32,(ST,BC),0)
    return jnp.where(io==ids,1.0,0.0).astype(BF16)

def gather(g3, oh, out):
    out[...]=jnp.dot(g3, jnp.concatenate([oh,oh,oh],0), preferred_element_type=F32)

def totals_body(gains, ants, m_ref, v_ref, d_ref, ga, gc, x_ref, acc, make_d):
    g3=jnp.concatenate(split3(gains),1)
    acc[...]=jnp.zeros_like(acc)
    def chunk(c, _):
        off=pl.multiple_of(c*BC,BC)
        oa=onehot(ants,0,off); oc=onehot(ants,1,off)
        gather(g3,oa,ga); gather(g3,oc,gc)
        for lt in range(BC//128):
            L=slice(lt*128,lt*128+128)
            D=pl.ds(pl.multiple_of(off+lt*128,128),128)
            res=[[v_ref[r,t,:,D] for r in range(2)] for t in range(2)]
            ps=[]
            for k in range(K):
                ra=slice(k*16,k*16+16); ia=slice(128+k*16,128+k*16+16)
                ar,ai,cr,ci=ga[ra,L],ga[ia,L],gc[ra,L],gc[ia,L]
                pr=ar*cr+ai*ci; pi=ai*cr-ar*ci
                ps.append((pr,pi))
                for t in range(2):
                    mr=m_ref[0,t,k,:,D].astype(F32); mi=m_ref[1,t,k,:,D].astype(F32)
                    res[t][0]=res[t][0]-(pr*mr-pi*mi)
                    res[t][1]=res[t][1]-(pr*mi+pi*mr)
            for k in range(K):
                ra=slice(k*16,k*16+16); ia=slice(128+k*16,128+k*16+16)
                ar,ai,cr,ci=ga[ra,L],ga[ia,L],gc[ra,L],gc[ia,L]
                pr,pi=ps[k]
                dd=0.0; qr=0.0; qi=0.0
                for t in range(2):
                    mr=m_ref[0,t,k,:,D].astype(F32); mi=m_ref[1,t,k,:,D].astype(F32)
                    rr,ri=res[t]
                    qr=qr+(rr*mr+ri*mi); qi=qi+(ri*mr-rr*mi)
                    if make_d: dd=dd+(mr*mr+mi*mi)
                if make_d: d_ref[k,:,D]=dd
                else: dd=d_ref[k,:,D]
                qr=qr+pr*dd; qi=qi+pi*dd
                vals=((qr*cr-qi*ci, qr*ci+qi*cr, (cr*cr+ci*ci)*dd),
                      (qr*ar+qi*ai, qr*ai-qi*ar, (ar*ar+ai*ai)*dd))
                for s in range(2):
                    LL=slice(s*BC+lt*128,s*BC+lt*128+128)
                    for q in range(3):
                        h,l=split2(vals[s][q])
                        x_ref[q*128+k*16:q*128+k*16+16,LL]=h
                        x_ref[384+q*128+k*16:384+q*128+k*16+16,LL]=l
        oh2=jnp.concatenate([oa,oc],1)
        t=lax.dot_general(x_ref[...],oh2,NT,preferred_element_type=F32)
        acc[...]+=t[:384]+t[384:]
        return 0
    lax.fori_loop(0,BL//BC,chunk,0)


def unpack(jp):
    return jnp.concatenate([jp[:, :ST], jp[:, ST:]], 0)


def pack(top, bottom):
    return jnp.concatenate([top, bottom], 1)


def first_kernel(g_ref, ants, m_ref, v_ref, d_ref, pay, ga, gc, x_ref, acc):
    totals_body(g_ref[...], ants, m_ref, v_ref, d_ref, ga, gc, x_ref, acc, True)
    inv = 1.0 / (acc[256:384, :] + RHO)
    bb = RHO * inv
    pay[pl.ds(0, 128, stride=3), :] = pack(g_ref[0:128, :], g_ref[128:256, :])
    pay[pl.ds(1, 128, stride=3), :] = pack(acc[0:128, :] * inv, acc[128:256, :] * inv)
    pay[pl.ds(2, 128, stride=3), :] = pack(bb, bb)


def fit_two_kernel(p_ref, x_ref, out):
    proj = p_ref[...]
    z0 = jnp.dot(proj, x_ref[pl.ds(0, 128, stride=3), :], precision=HIGH, preferred_element_type=F32)
    j1 = x_ref[pl.ds(1, 128, stride=3), :] + x_ref[pl.ds(2, 128, stride=3), :] * z0
    z1 = jnp.dot(proj, j1, precision=HIGH, preferred_element_type=F32)
    out[pl.ds(0, 128, stride=2), :] = z0
    out[pl.ds(1, 128, stride=2), :] = z1


def fit_kernel(p_ref, x_ref, out):
    out[...] = jnp.dot(p_ref[...], x_ref[...], precision=HIGH, preferred_element_type=F32)


def local_kernel(pay, z_ref, out):
    j1 = pay[pl.ds(1, 128, stride=3), :] + pay[pl.ds(2, 128, stride=3), :] * z_ref[pl.ds(0, 128, stride=2), :]
    z1 = z_ref[pl.ds(1, 128, stride=2), :]
    for h in range(CL):
        out[h * 256:h * 256 + 128, :] = j1
        out[h * 256 + 128:h * 256 + 256, :] = z1


def map_kernel(mine, theirs, t_ref, cnt):
    shared = mine.shape[1]
    io = lax.broadcasted_iota(jnp.int32, (ST, shared), 0)
    zero = jnp.zeros((ST, ST), F32)
    total = jnp.zeros((8, ST), F32)
    ones = jnp.ones((8, shared), BF16)
    for h in range(CL):
        om = jnp.where(io == mine[h:h + 1, :], 1.0, 0.0).astype(BF16)
        ot = jnp.where(io == theirs[h:h + 1, :], 1.0, 0.0).astype(BF16)
        t = lax.dot_general(ot, om, NT, preferred_element_type=F32)
        t_ref[h * 128:h * 128 + 128, :] = pack(jnp.concatenate([t, zero], 0), jnp.concatenate([zero, t], 0)).astype(BF16)
        total = total + lax.dot_general(ones, om, NT, preferred_element_type=F32)
    cnt[...] = 1.0 / (1.0 + pack(total, total))


def averaged(own, recv, t_ref, cnt):
    total = own
    for h in range(CL):
        t = t_ref[h * 128:h * 128 + 128, :]
        total = total + jnp.dot(jnp.concatenate(split3(recv[h]), 1), jnp.concatenate([t, t, t], 0), preferred_element_type=F32)
    return total * cnt[0:1, :]


def second_kernel(sent, recv, t_ref, cnt, ants, m_ref, v_ref, d_ref, out, ga, gc, x_ref, acc):
    both = averaged(sent[0:256, :], [recv[h * 256:h * 256 + 256, :] for h in range(CL)], t_ref, cnt)
    j1, z1 = both[:128], both[128:]
    totals_body(unpack(j1), ants, m_ref, v_ref, d_ref, ga, gc, x_ref, acc, False)
    inv = 1.0 / (acc[256:384, :] + RHO)
    num = pack(acc[0:128, :], acc[128:256, :])
    j2 = (num + RHO * (2.0 * z1 - j1)) * pack(inv, inv)
    for h in range(CL):
        out[h * 128:h * 128 + 128, :] = j2


def average_kernel(sent, recv, t_ref, cnt, out, rows):
    j2 = averaged(sent[0:128, :], [recv[h * 128:h * 128 + 128, :] for h in range(CL)], t_ref, cnt)
    out[...] = j2
    rows[...] = unpack(j2)


def unpack_kernel(z_ref, out):
    out[...] = unpack(z_ref[...])


def residual_kernel(g_ref, ants, m_ref, v_ref, out, ga, gc):
    g3=jnp.concatenate(split3(g_ref[...]),1)
    def chunk(c,_):
        off=pl.multiple_of(c*BC,BC)
        gather(g3,onehot(ants,0,off),ga); gather(g3,onehot(ants,1,off),gc)
        for lt in range(BC//128):
            L=slice(lt*128,lt*128+128)
            D=pl.ds(pl.multiple_of(off+lt*128,128),128)
            res=[[v_ref[r,t,:,D] for r in range(2)] for t in range(2)]
            for k in range(K):
                ra=slice(k*16,k*16+16); ia=slice(128+k*16,128+k*16+16)
                ar,ai,cr,ci=ga[ra,L],ga[ia,L],gc[ra,L],gc[ia,L]
                pr=ar*cr+ai*ci; pi=ai*cr-ar*ci
                for t in range(2):
                    mr=m_ref[0,t,k,:,D].astype(F32); mi=m_ref[1,t,k,:,D].astype(F32)
                    res[t][0]=res[t][0]-(pr*mr-pi*mi)
                    res[t][1]=res[t][1]-(pr*mi+pi*mr)
            for t in range(2):
                for r in range(2): out[r,t,:,D]=res[t][r]
        return 0
    lax.fori_loop(0,BL//BC,chunk,0)


def kernel(body, outs, ins, scratch=(), name=None, flops=1000000):
    return pl.pallas_call(
        body, out_shape=outs, in_specs=[VM] * ins,
        out_specs=(VM,) * len(outs) if isinstance(outs, tuple) else VM,
        scratch_shapes=list(scratch), name=name,
        cost_estimate=pl.CostEstimate(flops=flops, bytes_accessed=1000000, transcendentals=0))


def on_device(visibilities, model, flags, antennas, correlation, gains_init):
    keep = flags[0, 0] == 0
    m = jnp.where(keep[None, None], model[0][:, :, 0], jnp.zeros((), BF16)).transpose(0, 3, 1, 2, 4)
    v = jnp.where(keep[None], visibilities[0][:, 0], 0.0).transpose(0, 2, 1, 3)
    ants = antennas[0]
    gains = gains_init.reshape(2 * K * SI, ST)
    proj = jnp.asarray(projector())
    group = lax.axis_index("grp")
    mine = lax.dynamic_index_in_dim(correlation, group, 0, keepdims=False)
    theirs = lax.dynamic_index_in_dim(correlation, group, 1, keepdims=False)
    scratch = [pltpu.VMEM((256, BC), F32), pltpu.VMEM((256, BC), F32), pltpu.VMEM((768, 2 * BC), BF16), pltpu.VMEM((384, ST), F32)]
    exchange = functools.partial(lax.all_to_all, split_axis=0, concat_axis=0, tiled=True)

    big = 2000000000
    d, pay = kernel(first_kernel, (SD((K, SI, BL), F32), SD((384, 128), F32)), 4, scratch, "first", big)(gains, ants, m, v)
    tmap, cnt = kernel(map_kernel, (SD((CL * 128, 128), BF16), SD((8, 128), F32)), 2, name="maps")(mine, theirs)
    got = exchange(pay, "chan")
    z = kernel(fit_two_kernel, SD((256, 128), F32), 2, name="fits")(proj, got)
    z = exchange(z, "chan")
    sent = kernel(local_kernel, SD((CL * 256, 128), F32), 2, name="local")(pay, z)
    recv = exchange(sent, "grp")
    sent = kernel(second_kernel, SD((CL * 128, 128), F32), 8, scratch, "second", big)(sent, recv, tmap, cnt, ants, m, v, d)
    recv = exchange(sent, "grp")
    j2, rows = kernel(average_kernel, (SD((128, 128), F32), SD((256, ST), F32)), 4, name="average")(sent, recv, tmap, cnt)
    got = exchange(j2, "chan")
    res = kernel(residual_kernel, SD((2, 2, SI, BL), F32), 4, scratch[:2], "residual", big)(rows, ants, m, v)
    z = exchange(kernel(fit_kernel, SD((128, 128), F32), 2, name="fit")(proj, got), "chan")
    zrows = kernel(unpack_kernel, SD((256, ST), F32), 1, name="unpack")(z)
    shape = gains_init.shape
    return rows.reshape(shape), zrows.reshape(shape), res.transpose(0, 2, 1, 3)[None, :, None]


def solution(mesh):
    return jax.shard_map(
        on_device,
        mesh=mesh,
        in_specs=(
            P("grp", None, "chan", None, None, None),
            P("grp", None, None, "chan", None, None, None),
            P("grp", "chan", None, None, None),
            P("grp", None, None),
            P(),
            P("grp", None, None, "chan", None, None),
        ),
        out_specs=(
            P("grp", None, None, "chan", None, None),
            P("grp", None, None, "chan", None, None),
            P("grp", None, "chan", None, None, None),
        ),
        check_vma=False,
    )
```

```python
import functools

import jax
import jax.numpy as jnp
import numpy as np
from jax import lax
from jax.experimental import pallas as pl
from jax.experimental.pallas import tpu as pltpu
from jax.sharding import Mesh, PartitionSpec as P

K, SI, ST, BL, CL, CH = 8, 16, 64, 2048, 4, 128
RHO = 128.0
F32, BF16 = jnp.float32, jnp.bfloat16
NT = (((1,), (1,)), ((), ()))
HIGH = lax.Precision.HIGHEST
BC = 256
VM = pl.BlockSpec(memory_space=pltpu.VMEM)
SD = jax.ShapeDtypeStruct
CUBE = ("y", "zl", "c")


def fit_tables():
    f = np.arange(CH, dtype=np.float64)
    x = (2 * f + 1) / CH - 1
    basis = np.stack([np.ones_like(x), x, 1.5 * x * x - 0.5], axis=1)
    inverse = np.linalg.inv(basis.T @ basis)
    order = np.arange(CH).reshape(4, 4, 4, 2).transpose(1, 0, 2, 3).reshape(4, 32)
    down, up = [], []
    for part in order:
        b = np.zeros((32, 4))
        b[:, :3] = basis[part]
        w = np.zeros((4, 32))
        w[:3] = inverse @ basis[part].T
        down.append(np.kron(w, np.eye(4)))
        up.append(np.kron(b, np.eye(4)))
    return np.concatenate(down).astype(np.float32), np.concatenate(up).astype(np.float32)


def split3(x):
    hi=x.astype(BF16); r=x-hi.astype(F32); mid=r.astype(BF16); lo=(r-mid.astype(F32)).astype(BF16)
    return hi,mid,lo

def split2(x):
    hi=x.astype(BF16)
    return hi,(x-hi.astype(F32)).astype(BF16)

def onehot(ants, side, off):
    ids=ants[side:side+1, pl.ds(off,BC)]
    io=lax.broadcasted_iota(jnp.int32,(ST,BC),0)
    return jnp.where(io==ids,1.0,0.0).astype(BF16)

def gather(g3, oh, out):
    out[...]=jnp.dot(g3, jnp.concatenate([oh,oh,oh],0), preferred_element_type=F32)

def totals_body(gains, ants, m_ref, v_ref, d_ref, ga, gc, x_ref, acc, make_d):
    g3=jnp.concatenate(split3(gains),1)
    acc[...]=jnp.zeros_like(acc)
    def chunk(c, _):
        off=pl.multiple_of(c*BC,BC)
        oa=onehot(ants,0,off); oc=onehot(ants,1,off)
        gather(g3,oa,ga); gather(g3,oc,gc)
        for lt in range(BC//128):
            L=slice(lt*128,lt*128+128)
            D=pl.ds(pl.multiple_of(off+lt*128,128),128)
            res=[[v_ref[r,t,:,D] for r in range(2)] for t in range(2)]
            ps=[]
            for k in range(K):
                ra=slice(k*16,k*16+16); ia=slice(128+k*16,128+k*16+16)
                ar,ai,cr,ci=ga[ra,L],ga[ia,L],gc[ra,L],gc[ia,L]
                pr=ar*cr+ai*ci; pi=ai*cr-ar*ci
                ps.append((pr,pi))
                for t in range(2):
                    mr=m_ref[0,t,k,:,D].astype(F32); mi=m_ref[1,t,k,:,D].astype(F32)
                    res[t][0]=res[t][0]-(pr*mr-pi*mi)
                    res[t][1]=res[t][1]-(pr*mi+pi*mr)
            for k in range(K):
                ra=slice(k*16,k*16+16); ia=slice(128+k*16,128+k*16+16)
                ar,ai,cr,ci=ga[ra,L],ga[ia,L],gc[ra,L],gc[ia,L]
                pr,pi=ps[k]
                dd=0.0; qr=0.0; qi=0.0
                for t in range(2):
                    mr=m_ref[0,t,k,:,D].astype(F32); mi=m_ref[1,t,k,:,D].astype(F32)
                    rr,ri=res[t]
                    qr=qr+(rr*mr+ri*mi); qi=qi+(ri*mr-rr*mi)
                    if make_d: dd=dd+(mr*mr+mi*mi)
                if make_d: d_ref[k,:,D]=dd
                else: dd=d_ref[k,:,D]
                qr=qr+pr*dd; qi=qi+pi*dd
                vals=((qr*cr-qi*ci, qr*ci+qi*cr, (cr*cr+ci*ci)*dd),
                      (qr*ar+qi*ai, qr*ai-qi*ar, (ar*ar+ai*ai)*dd))
                for s in range(2):
                    LL=slice(s*BC+lt*128,s*BC+lt*128+128)
                    for q in range(3):
                        h,l=split2(vals[s][q])
                        x_ref[q*128+k*16:q*128+k*16+16,LL]=h
                        x_ref[384+q*128+k*16:384+q*128+k*16+16,LL]=l
        oh2=jnp.concatenate([oa,oc],1)
        t=lax.dot_general(x_ref[...],oh2,NT,preferred_element_type=F32)
        acc[...]+=t[:384]+t[384:]
        return 0
    lax.fori_loop(0,BL//BC,chunk,0)


def unpack(jp):
    return jnp.concatenate([jp[:, :ST], jp[:, ST:]], 0)


def pack(top, bottom):
    return jnp.concatenate([top, bottom], 1)


def pack_kernel(g_ref, out):
    out[...] = pack(g_ref[0:128, :], g_ref[128:256, :])


def merge(out, fit, tmp, ab):
    tmp[...] = fit
    for r in range(4):
        at = pl.ds(r, 32, stride=4)
        out[pl.ds(r, 32, stride=16), :] = tmp[at, :]
        out[pl.ds(4 + r, 32, stride=16), :] = ab[at, :]
        out[pl.ds(8 + r, 32, stride=16), :] = ab[pl.ds(128 + r, 32, stride=4), :]


def copies(out, value, times):
    rows = value.shape[0]
    for i in range(times):
        out[i * rows:i * rows + rows, :] = value


def first_kernel(g_ref, ants, m_ref, v_ref, d_ref, ab, ga, gc, x_ref, acc):
    totals_body(g_ref[...], ants, m_ref, v_ref, d_ref, ga, gc, x_ref, acc, True)
    inv = 1.0 / (acc[256:384, :] + RHO)
    inv = pack(inv, inv)
    ab[0:128, :] = pack(acc[0:128, :], acc[128:256, :]) * inv
    ab[128:256, :] = RHO * inv


def table(ref, rows):
    return ref[pl.ds(pl.multiple_of(lax.axis_index("zh") * rows, rows), rows), :]


def mm(a, b):
    return jnp.dot(a, b, precision=HIGH, preferred_element_type=F32)


def part_kernel(down, recv, out):
    copies(out, mm(table(down, 16), recv[...]), 4)


def fit_kernel(up, recv, ab, out, zh, tmp):
    z = mm(table(up, 128), recv[0:16, :] + recv[16:32, :] + recv[32:48, :] + recv[48:64, :])
    zh[...] = z
    merge(out, z, tmp, ab)


def coefficients(recv, t_ref, cnt):
    parts = []
    for h in range(CL):
        s = h * 64
        parts.append(recv[s:s + 16, :] + recv[s + 16:s + 32, :] + recv[s + 32:s + 48, :] + recv[s + 48:s + 64, :])
    return averaged(parts, range(CL), t_ref, cnt)


def fit_average_kernel(up, recv, t_ref, cnt, ab, out, zh, tmp):
    z = mm(table(up, 128), coefficients(recv, t_ref, cnt))
    zh[...] = z
    merge(out, z, tmp, ab)


def last_fit_kernel(up, recv, t_ref, cnt, out):
    out[...] = mm(table(up, 128), coefficients(recv, t_ref, cnt))


def update_kernel(down, got, zh, ab, part, j_out, tmp):
    for r in range(4):
        at = pl.ds(r, 32, stride=4)
        tmp[at, :] = got[pl.ds(4 + r, 32, stride=16), :] + got[pl.ds(8 + r, 32, stride=16), :] * zh[at, :]
        j_out[at, :] = ab[at, :] + ab[pl.ds(128 + r, 32, stride=4), :] * got[pl.ds(r, 32, stride=16), :]
    copies(part, mm(table(down, 16), tmp[...]), 16)


def map_kernel(mine, theirs, own, t_ref, cnt):
    shared = mine.shape[1]
    io = lax.broadcasted_iota(jnp.int32, (ST, shared), 0)
    eye = jnp.where(lax.broadcasted_iota(jnp.int32, (ST, ST), 0) == lax.broadcasted_iota(jnp.int32, (ST, ST), 1), 1.0, 0.0)
    zero = jnp.zeros((ST, ST), F32)
    total = jnp.zeros((8, ST), F32)
    ones = jnp.ones((8, shared), BF16)
    for h in range(CL):
        om = jnp.where(io == mine[h:h + 1, :], 1.0, 0.0).astype(BF16)
        ot = jnp.where(io == theirs[h:h + 1, :], 1.0, 0.0).astype(BF16)
        t = lax.dot_general(ot, om, NT, preferred_element_type=F32) + eye * own[h:h + 1, :]
        t_ref[h * 128:h * 128 + 128, :] = pack(jnp.concatenate([t, zero], 0), jnp.concatenate([zero, t], 0)).astype(BF16)
        total = total + lax.dot_general(ones, om, NT, preferred_element_type=F32)
    cnt[...] = 1.0 / (1.0 + pack(total, total))


def averaged(parts, clusters, t_ref, cnt):
    total = 0.0
    for x, h in zip(parts, clusters):
        t = t_ref[pl.ds(pl.multiple_of(h * 128, 128), 128), :]
        total = total + jnp.dot(jnp.concatenate(split3(x), 1), jnp.concatenate([t, t, t], 0), preferred_element_type=F32)
    return total * cnt[0:1, :]


def average_of(own, r1, r2, r3, t_ref, cnt):
    g = lax.axis_index("x")
    return averaged([own[...], r1[...], r2[...], r3[...]], [lax.rem(g + CL - s, CL) for s in range(CL)], t_ref, cnt)


def second_kernel(own, r1, r2, r3, t_ref, cnt, ants, m_ref, v_ref, d_ref, ab, ga, gc, x_ref, acc):
    j1 = average_of(own, r1, r2, r3, t_ref, cnt)
    totals_body(unpack(j1), ants, m_ref, v_ref, d_ref, ga, gc, x_ref, acc, False)
    inv = 1.0 / (acc[256:384, :] + RHO)
    inv = pack(inv, inv)
    ab[0:128, :] = (pack(acc[0:128, :], acc[128:256, :]) - RHO * j1) * inv
    ab[128:256, :] = (2.0 * RHO) * inv


def unpack_kernel(z_ref, out):
    out[...] = unpack(z_ref[...])


def residual_kernel(own, r1, r2, r3, t_ref, cnt, ants, m_ref, v_ref, rows, out, ga, gc):
    gains = unpack(average_of(own, r1, r2, r3, t_ref, cnt))
    rows[...] = gains
    g3 = jnp.concatenate(split3(gains), 1)
    def chunk(c,_):
        off=pl.multiple_of(c*BC,BC)
        gather(g3,onehot(ants,0,off),ga); gather(g3,onehot(ants,1,off),gc)
        for lt in range(BC//128):
            L=slice(lt*128,lt*128+128)
            D=pl.ds(pl.multiple_of(off+lt*128,128),128)
            res=[[v_ref[r,t,:,D] for r in range(2)] for t in range(2)]
            for k in range(K):
                ra=slice(k*16,k*16+16); ia=slice(128+k*16,128+k*16+16)
                ar,ai,cr,ci=ga[ra,L],ga[ia,L],gc[ra,L],gc[ia,L]
                pr=ar*cr+ai*ci; pi=ai*cr-ar*ci
                for t in range(2):
                    mr=m_ref[0,t,k,:,D].astype(F32); mi=m_ref[1,t,k,:,D].astype(F32)
                    res[t][0]=res[t][0]-(pr*mr-pi*mi)
                    res[t][1]=res[t][1]-(pr*mi+pi*mr)
            for t in range(2):
                for r in range(2): out[r,t,:,D]=res[t][r]
        return 0
    lax.fori_loop(0,BL//BC,chunk,0)


def kernel(body, outs, ins, scratch=(), name=None, flops=100000000, vmem=8):
    return pl.pallas_call(
        body, out_shape=outs, in_specs=[VM] * ins,
        out_specs=(VM,) * len(outs) if isinstance(outs, tuple) else VM,
        scratch_shapes=list(scratch), name=name,
        compiler_params=pltpu.CompilerParams(vmem_limit_bytes=vmem * 1048576),
        cost_estimate=pl.CostEstimate(flops=flops, bytes_accessed=1000000, transcendentals=0))


def on_device(visibilities, model, flags, antennas, correlation, gains_init):
    ants = antennas[0]
    gains = gains_init.reshape(2 * K * SI, ST)
    down, up = (jnp.asarray(t) for t in fit_tables())
    group = lax.axis_index("x")
    mine = lax.dynamic_index_in_dim(correlation, group, 0, keepdims=False)
    theirs = lax.dynamic_index_in_dim(correlation, group, 1, keepdims=False)
    own = jnp.broadcast_to(jnp.where(jnp.arange(CL) == group, 1.0, 0.0)[:, None], (CL, ST))
    full = SD((128, 128), F32)
    tile = pltpu.VMEM((128, 128), F32)
    exchange = functools.partial(lax.all_to_all, split_axis=0, concat_axis=0, tiled=True)
    scratch = [pltpu.VMEM((256, BC), F32), pltpu.VMEM((256, BC), F32), pltpu.VMEM((768, 2 * BC), BF16), pltpu.VMEM((384, ST), F32)]
    big = 2000000000
    wide = SD((512, 128), F32)
    pairs = SD((256, 128), F32)

    def others(j):
        return [lax.ppermute(j, "x", [(i, (i + s) % CL) for i in range(CL)]) for s in range(1, CL)]

    j0 = kernel(pack_kernel, full, 1, name="pack")(gains)
    got = exchange(j0, CUBE)
    part = kernel(part_kernel, SD((64, 128), F32), 2, name="part")(down, got)
    got = exchange(part, "zh")

    keep = flags[0, 0] == 0
    m = jnp.where(keep[None, None], model[0][:, :, 0], jnp.zeros((), BF16)).transpose(0, 3, 1, 2, 4)
    v = jnp.where(keep[None], visibilities[0][:, 0], 0.0).transpose(0, 2, 1, 3)
    tmap, cnt = kernel(map_kernel, (SD((CL * 128, 128), BF16), SD((8, 128), F32)), 3, name="maps")(mine, theirs, own)
    d, ab = kernel(first_kernel, (SD((K, SI, BL), F32), pairs), 4, scratch, "first", big, 24)(gains, ants, m, v)

    send, zh = kernel(fit_kernel, (wide, full), 3, [tile], "fit")(up, got, ab)
    got = exchange(send, CUBE)
    part, j1 = kernel(update_kernel, (pairs, full), 4, [tile], "update")(down, got, zh, ab)
    got = exchange(part, ("x", "zh"))
    d1 = others(j1)
    ab = kernel(second_kernel, pairs, 10, scratch, "second", big, 24)(j1, *d1, tmap, cnt, ants, m, v, d)
    send, zh = kernel(fit_average_kernel, (wide, full), 5, [tile], "fits")(up, got, tmap, cnt, ab)
    got = exchange(send, CUBE)
    part, j2 = kernel(update_kernel, (pairs, full), 4, [tile], "update2")(down, got, zh, ab)
    got = exchange(part, ("x", "zh"))
    d2 = others(j2)
    rows, res = kernel(residual_kernel, (SD((256, ST), F32), SD((2, 2, SI, BL), F32)), 9, scratch[:2], "residual", big, 24)(
        j2, *d2, tmap, cnt, ants, m, v)
    z = kernel(last_fit_kernel, full, 4, name="lastfit")(up, got, tmap, cnt)
    zrows = kernel(unpack_kernel, SD((256, ST), F32), 1, name="unpack")(exchange(z, CUBE))
    shape = gains_init.shape
    return rows.reshape(shape), zrows.reshape(shape), res.transpose(0, 2, 1, 3)[None, :, None]


def solution(mesh):
    split = Mesh(mesh.devices.reshape(4, 4, 4, 4, 2), ("x", "y", "zh", "zl", "c"))
    chan = ("y", "zh", "zl", "c")
    return jax.shard_map(
        on_device,
        mesh=split,
        in_specs=(
            P("x", None, chan, None, None, None),
            P("x", None, None, chan, None, None, None),
            P("x", chan, None, None, None),
            P("x", None, None),
            P(),
            P("x", None, None, chan, None, None),
        ),
        out_specs=(
            P("x", None, None, chan, None, None),
            P("x", None, None, chan, None, None),
            P("x", None, chan, None, None, None),
        ),
        check_vma=False,
    )
```

```python
import functools

import jax
import jax.numpy as jnp
import numpy as np
from jax import lax
from jax.experimental import pallas as pl
from jax.experimental.pallas import tpu as pltpu
from jax.sharding import Mesh, PartitionSpec as P

K, SI, ST, BL, CL, CH = 8, 16, 64, 2048, 4, 128
RHO = 128.0
F32, BF16 = jnp.float32, jnp.bfloat16
NT = (((1,), (1,)), ((), ()))
HIGH = lax.Precision.HIGHEST
BC = 512
VM = pl.BlockSpec(memory_space=pltpu.VMEM)
SD = jax.ShapeDtypeStruct
CUBE = ("y", "zl", "c")
CHAN = ("y", "zh", "zl", "c")


def fit_tables():
    f = np.arange(CH, dtype=np.float64)
    x = (2 * f + 1) / CH - 1
    basis = np.stack([np.ones_like(x), x, 1.5 * x * x - 0.5], axis=1)
    inverse = np.linalg.inv(basis.T @ basis)
    order = np.arange(CH).reshape(4, 4, 4, 2).transpose(1, 0, 2, 3).reshape(4, 32)
    down, up = [], []
    for part in order:
        b = np.zeros((32, 4))
        b[:, :3] = basis[part]
        w = np.zeros((4, 32))
        w[:3] = inverse @ basis[part].T
        down.append(np.kron(w, np.eye(4)))
        up.append(np.kron(b, np.eye(4)))
    whole = np.zeros((4, CH))
    whole[:3] = inverse @ basis.T
    return (np.kron(whole, np.eye(4)).astype(np.float32), np.concatenate(down).astype(np.float32),
            np.concatenate(up).astype(np.float32))


def split3(x):
    hi=x.astype(BF16); r=x-hi.astype(F32); mid=r.astype(BF16); lo=(r-mid.astype(F32)).astype(BF16)
    return hi,mid,lo

def split2(x):
    hi=x.astype(BF16)
    return hi,(x-hi.astype(F32)).astype(BF16)

def onehot(ants, side, off):
    ids=ants[side:side+1, pl.ds(off,BC)]
    io=lax.broadcasted_iota(jnp.int32,(ST,BC),0)
    return jnp.where(io==ids,1.0,0.0).astype(BF16)

def gather(g3, oh, out):
    out[...]=jnp.dot(g3, jnp.concatenate([oh,oh,oh],0), preferred_element_type=F32)

def totals_body(gains, ants, m_ref, v_ref, ga, gc, x_ref, acc):
    g3=jnp.concatenate(split3(gains),1)
    acc[...]=jnp.zeros_like(acc)
    def chunk(c, _):
        off=pl.multiple_of(c*BC,BC)
        oa=onehot(ants,0,off); oc=onehot(ants,1,off)
        gather(g3,oa,ga); gather(g3,oc,gc)
        for lt in range(BC//128):
            L=slice(lt*128,lt*128+128)
            D=pl.ds(pl.multiple_of(off+lt*128,128),128)
            res=[[v_ref[r,t,:,D] for r in range(2)] for t in range(2)]
            ps=[]
            for k in range(K):
                ra=slice(k*16,k*16+16); ia=slice(128+k*16,128+k*16+16)
                ar,ai,cr,ci=ga[ra,L],ga[ia,L],gc[ra,L],gc[ia,L]
                pr=ar*cr+ai*ci; pi=ai*cr-ar*ci
                ps.append((pr,pi))
                for t in range(2):
                    mr=m_ref[0,t,k,:,D].astype(F32); mi=m_ref[1,t,k,:,D].astype(F32)
                    res[t][0]=res[t][0]-(pr*mr-pi*mi)
                    res[t][1]=res[t][1]-(pr*mi+pi*mr)
            for k in range(K):
                ra=slice(k*16,k*16+16); ia=slice(128+k*16,128+k*16+16)
                ar,ai,cr,ci=ga[ra,L],ga[ia,L],gc[ra,L],gc[ia,L]
                pr,pi=ps[k]
                dd=0.0; qr=0.0; qi=0.0
                for t in range(2):
                    mr=m_ref[0,t,k,:,D].astype(F32); mi=m_ref[1,t,k,:,D].astype(F32)
                    rr,ri=res[t]
                    qr=qr+(rr*mr+ri*mi); qi=qi+(ri*mr-rr*mi)
                    dd=dd+(mr*mr+mi*mi)
                qr=qr+pr*dd; qi=qi+pi*dd
                vals=((qr*cr-qi*ci, qr*ci+qi*cr, (cr*cr+ci*ci)*dd),
                      (qr*ar+qi*ai, qr*ai-qi*ar, (ar*ar+ai*ai)*dd))
                for s in range(2):
                    LL=slice(s*BC+lt*128,s*BC+lt*128+128)
                    for q in range(3):
                        h,l=split2(vals[s][q])
                        x_ref[q*128+k*16:q*128+k*16+16,LL]=h
                        x_ref[384+q*128+k*16:384+q*128+k*16+16,LL]=l
        oh2=jnp.concatenate([oa,oc],1)
        t=lax.dot_general(x_ref[...],oh2,NT,preferred_element_type=F32)
        acc[...]+=t[:384]+t[384:]
        return 0
    lax.fori_loop(0,BL//BC,chunk,0,unroll=2)


def unpack(jp):
    return jnp.concatenate([jp[:, :ST], jp[:, ST:]], 0)


def pack(top, bottom):
    return jnp.concatenate([top, bottom], 1)


def pack_kernel(g_ref, out):
    j = pack(g_ref[0:128, :], g_ref[128:256, :])
    for y in range(4):
        for cube in range(4):
            out[y * 128 + cube * 32:y * 128 + cube * 32 + 32, :] = j[y * 32:y * 32 + 32, :]


def merge(out, fit, tmp, ab):
    tmp[...] = fit
    for r in range(4):
        at = pl.ds(r, 32, stride=4)
        out[pl.ds(r, 32, stride=16), :] = tmp[at, :]
        out[pl.ds(4 + r, 32, stride=16), :] = ab[at, :]
        out[pl.ds(8 + r, 32, stride=16), :] = ab[pl.ds(128 + r, 32, stride=4), :]


def copies(out, value, times):
    rows = value.shape[0]
    for i in range(times):
        out[i * rows:i * rows + rows, :] = value


def first_kernel(g_ref, ants, m_ref, v_ref, ab, ga, gc, x_ref, acc):
    totals_body(g_ref[...], ants, m_ref, v_ref, ga, gc, x_ref, acc)
    inv = 1.0 / (acc[256:384, :] + RHO)
    inv = pack(inv, inv)
    ab[0:128, :] = pack(acc[0:128, :], acc[128:256, :]) * inv
    ab[128:256, :] = RHO * inv


def table(ref, rows):
    return ref[pl.ds(pl.multiple_of(lax.axis_index("zh") * rows, rows), rows), :]


def mm(a, b):
    return jnp.dot(a, b, precision=HIGH, preferred_element_type=F32)


def fit_kernel(whole, up, recv, ab, out, zh, tmp):
    z = mm(table(up, 128), mm(whole[...], recv[...]))
    zh[...] = z
    merge(out, z, tmp, ab)


def coefficients(recv, t_ref, cnt):
    parts = []
    for h in range(CL):
        s = h * 64
        parts.append(recv[s:s + 16, :] + recv[s + 16:s + 32, :] + recv[s + 32:s + 48, :] + recv[s + 48:s + 64, :])
    return averaged(parts, range(CL), t_ref, cnt)


def fit_average_kernel(up, recv, t_ref, cnt, ab, out, zh, tmp):
    z = mm(table(up, 128), coefficients(recv, t_ref, cnt))
    zh[...] = z
    merge(out, z, tmp, ab)


def last_fit_kernel(up, recv, t_ref, cnt, out):
    out[...] = mm(table(up, 128), coefficients(recv, t_ref, cnt))


def update_kernel(spread, down, got, zh, ab, part, j_out, tmp):
    for r in range(4):
        at = pl.ds(r, 32, stride=4)
        tmp[at, :] = got[pl.ds(4 + r, 32, stride=16), :] + got[pl.ds(8 + r, 32, stride=16), :] * zh[at, :]
        j_out[at, :] = ab[at, :] + ab[pl.ds(128 + r, 32, stride=4), :] * got[pl.ds(r, 32, stride=16), :]
    copies(part, mm(table(down, 16), tmp[...]), 16)
    for i in range(1, spread):
        j_out[i * 128:i * 128 + 128, :] = j_out[0:128, :]


def map_kernel(mine, theirs, own, t_ref, cnt):
    shared = mine.shape[1]
    io = lax.broadcasted_iota(jnp.int32, (ST, shared), 0)
    eye = jnp.where(lax.broadcasted_iota(jnp.int32, (ST, ST), 0) == lax.broadcasted_iota(jnp.int32, (ST, ST), 1), 1.0, 0.0)
    zero = jnp.zeros((ST, ST), F32)
    total = jnp.zeros((8, ST), F32)
    ones = jnp.ones((8, shared), BF16)
    for h in range(CL):
        om = jnp.where(io == mine[h:h + 1, :], 1.0, 0.0).astype(BF16)
        ot = jnp.where(io == theirs[h:h + 1, :], 1.0, 0.0).astype(BF16)
        t = lax.dot_general(ot, om, NT, preferred_element_type=F32) + eye * own[h:h + 1, :]
        t_ref[h * 128:h * 128 + 128, :] = pack(jnp.concatenate([t, zero], 0), jnp.concatenate([zero, t], 0)).astype(BF16)
        total = total + lax.dot_general(ones, om, NT, preferred_element_type=F32)
    cnt[...] = 1.0 / (1.0 + pack(total, total))


def averaged(parts, clusters, t_ref, cnt):
    total = 0.0
    for x, h in zip(parts, clusters):
        t = t_ref[pl.ds(pl.multiple_of(h * 128, 128), 128), :]
        total = total + jnp.dot(jnp.concatenate(split3(x), 1), jnp.concatenate([t, t, t], 0), preferred_element_type=F32)
    return total * cnt[0:1, :]


def average_of(own, r1, r2, r3, t_ref, cnt):
    g = lax.axis_index("x")
    return averaged([own[...], r1[...], r2[...], r3[...]], [lax.rem(g + CL - s, CL) for s in range(CL)], t_ref, cnt)


def second_kernel(recv, t_ref, cnt, ants, m_ref, v_ref, ab, ga, gc, x_ref, acc):
    j1 = averaged([recv[h * 128:h * 128 + 128, :] for h in range(CL)], range(CL), t_ref, cnt)
    totals_body(unpack(j1), ants, m_ref, v_ref, ga, gc, x_ref, acc)
    inv = 1.0 / (acc[256:384, :] + RHO)
    inv = pack(inv, inv)
    ab[0:128, :] = (pack(acc[0:128, :], acc[128:256, :]) - RHO * j1) * inv
    ab[128:256, :] = (2.0 * RHO) * inv


def unpack_kernel(z_ref, out):
    out[...] = unpack(z_ref[...])


def residual_kernel(own, r1, r2, r3, t_ref, cnt, ants, m_ref, v_ref, rows, out, ga, gc):
    gains = unpack(average_of(own, r1, r2, r3, t_ref, cnt))
    rows[...] = gains
    g3 = jnp.concatenate(split3(gains), 1)
    def chunk(c,_):
        off=pl.multiple_of(c*BC,BC)
        gather(g3,onehot(ants,0,off),ga); gather(g3,onehot(ants,1,off),gc)
        for lt in range(BC//128):
            L=slice(lt*128,lt*128+128)
            D=pl.ds(pl.multiple_of(off+lt*128,128),128)
            res=[[v_ref[r,t,:,D] for r in range(2)] for t in range(2)]
            for k in range(K):
                ra=slice(k*16,k*16+16); ia=slice(128+k*16,128+k*16+16)
                ar,ai,cr,ci=ga[ra,L],ga[ia,L],gc[ra,L],gc[ia,L]
                pr=ar*cr+ai*ci; pi=ai*cr-ar*ci
                for t in range(2):
                    mr=m_ref[0,t,k,:,D].astype(F32); mi=m_ref[1,t,k,:,D].astype(F32)
                    res[t][0]=res[t][0]-(pr*mr-pi*mi)
                    res[t][1]=res[t][1]-(pr*mi+pi*mr)
            for t in range(2):
                for r in range(2): out[r,t,:,D]=res[t][r]
        return 0
    lax.fori_loop(0,BL//BC,chunk,0,unroll=2)


def kernel(body, outs, ins, scratch=(), name=None, flops=100000000, vmem=8):
    return pl.pallas_call(
        body, out_shape=outs, in_specs=[VM] * ins,
        out_specs=(VM,) * len(outs) if isinstance(outs, tuple) else VM,
        scratch_shapes=list(scratch), name=name,
        compiler_params=pltpu.CompilerParams(vmem_limit_bytes=vmem * 1048576),
        cost_estimate=pl.CostEstimate(flops=flops, bytes_accessed=1000000, transcendentals=0))


def on_device(visibilities, model, flags, antennas, correlation, gains_init):
    ants = antennas[0]
    gains = gains_init.reshape(2 * K * SI, ST)
    whole, down, up = (jnp.asarray(t) for t in fit_tables())
    group = lax.axis_index("x")
    mine = lax.dynamic_index_in_dim(correlation, group, 0, keepdims=False)
    theirs = lax.dynamic_index_in_dim(correlation, group, 1, keepdims=False)
    own = jnp.broadcast_to(jnp.where(jnp.arange(CL) == group, 1.0, 0.0)[:, None], (CL, ST))
    full = SD((128, 128), F32)
    tile = pltpu.VMEM((128, 128), F32)
    exchange = functools.partial(lax.all_to_all, split_axis=0, concat_axis=0, tiled=True)
    scratch = [pltpu.VMEM((256, BC), F32), pltpu.VMEM((256, BC), F32), pltpu.VMEM((768, 2 * BC), BF16), pltpu.VMEM((384, ST), F32)]
    big = 2000000000
    wide = SD((512, 128), F32)
    pairs = SD((256, 128), F32)

    def others(j):
        return [lax.ppermute(j, "x", [(i, (i + s) % CL) for i in range(CL)]) for s in range(1, CL)]

    got = exchange(kernel(pack_kernel, wide, 1, name="pack")(gains), CHAN)

    keep = flags[0, 0] == 0
    m = jnp.where(keep[None, None], model[0][:, :, 0], jnp.zeros((), BF16)).transpose(0, 3, 1, 2, 4)
    v = jnp.where(keep[None], visibilities[0][:, 0], 0.0).transpose(0, 2, 1, 3)
    tmap, cnt = kernel(map_kernel, (SD((CL * 128, 128), BF16), SD((8, 128), F32)), 3, name="maps")(mine, theirs, own)
    ab = kernel(first_kernel, pairs, 4, scratch, "first", big, 24)(gains, ants, m, v)

    got, tmap, cnt, ab = lax.optimization_barrier((got, tmap, cnt, ab))
    send, zh = kernel(fit_kernel, (wide, full), 4, [tile], "fit")(whole, up, got, ab)
    got = exchange(send, CUBE)
    part, j1 = kernel(functools.partial(update_kernel, CL), (pairs, wide), 4, [tile], "update")(down, got, zh, ab)
    recv = exchange(j1, "x")
    recv, part = lax.optimization_barrier((recv, part))
    got = exchange(part, ("x", "zh"))
    ab = kernel(second_kernel, pairs, 6, scratch, "second", big, 24)(recv, tmap, cnt, ants, m, v)
    send, zh = kernel(fit_average_kernel, (wide, full), 5, [tile], "fits")(up, got, tmap, cnt, ab)
    got = exchange(send, CUBE)
    part, j2 = kernel(functools.partial(update_kernel, 1), (pairs, full), 4, [tile], "update2")(down, got, zh, ab)
    got = exchange(part, ("x", "zh"))
    d2 = others(j2)
    got, *d2 = lax.optimization_barrier((got, *d2))
    rows, res = kernel(residual_kernel, (SD((256, ST), F32), SD((2, 2, SI, BL), F32)), 9, scratch[:2], "residual", big, 24)(
        j2, *d2, tmap, cnt, ants, m, v)
    z = kernel(last_fit_kernel, full, 4, name="lastfit")(up, got, tmap, cnt)
    zrows = kernel(unpack_kernel, SD((256, ST), F32), 1, name="unpack")(exchange(z, CUBE))
    shape = gains_init.shape
    return rows.reshape(shape), zrows.reshape(shape), res.transpose(0, 2, 1, 3)[None, :, None]


def solution(mesh):
    split = Mesh(mesh.devices.reshape(4, 4, 4, 4, 2), ("x", "y", "zh", "zl", "c"))
    return jax.shard_map(
        on_device,
        mesh=split,
        in_specs=(
            P("x", None, CHAN, None, None, None),
            P("x", None, None, CHAN, None, None, None),
            P("x", CHAN, None, None, None),
            P("x", None, None),
            P(),
            P("x", None, None, CHAN, None, None),
        ),
        out_specs=(
            P("x", None, None, CHAN, None, None),
            P("x", None, None, CHAN, None, None),
            P("x", None, CHAN, None, None, None),
        ),
        check_vma=False,
    )
```

```python
import functools

import jax
import jax.numpy as jnp
import numpy as np
from jax import lax
from jax.experimental import pallas as pl
from jax.experimental.pallas import tpu as pltpu
from jax.sharding import Mesh, PartitionSpec as P

K, SI, ST, BL, CL, CH = 8, 16, 64, 2048, 4, 128
RHO = 128.0
F32, BF16 = jnp.float32, jnp.bfloat16
NT = (((1,), (1,)), ((), ()))
HIGH = lax.Precision.HIGHEST
BC = 512
VM = pl.BlockSpec(memory_space=pltpu.VMEM)
SD = jax.ShapeDtypeStruct
CUBE = ("y", "c", "zl")
PLANE = ("y", "c")
CHAN = ("y", "zh", "zl", "c")


def inverse_gram():
    f = np.arange(CH, dtype=np.float64)
    x = (2 * f + 1) / CH - 1
    basis = np.stack([np.ones_like(x), x, 1.5 * x * x - 0.5], axis=1)
    return np.linalg.inv(basis.T @ basis)


GINV = inverse_gram()


def iota(shape, dim):
    return lax.broadcasted_iota(jnp.int32, shape, dim)


def position(y, z, c):
    return (2 * (y * 32 + z * 2 + c) + 1).astype(F32) * (1.0 / CH) - 1.0


def basis_value(n, x):
    return jnp.where(n == 0, 1.0, jnp.where(n == 1, x, jnp.where(n == 2, 1.5 * x * x - 0.5, 0.0)))


def weight_value(n, x):
    second = 1.5 * x * x - 0.5
    rows = [float(g[0]) + float(g[1]) * x + float(g[2]) * second for g in GINV]
    return jnp.where(n == 0, rows[0], jnp.where(n == 1, rows[1], jnp.where(n == 2, rows[2], 0.0)))


def cube_entry(value, j, q):
    x = position(q >> 5, lax.axis_index("zh") * 4 + ((q >> 2) & 3), (q >> 4) & 1)
    return jnp.where((j & 3) == (q & 3), value(j >> 2, x), 0.0)


def cube_down():
    return cube_entry(weight_value, iota((16, 128), 0), iota((16, 128), 1))


def cube_up():
    return cube_entry(basis_value, iota((128, 16), 1), iota((128, 16), 0))


def plane_down():
    j, q = iota((48, 128), 0), iota((48, 128), 1)
    zl = (j * 43) >> 9
    j = j - zl * 12
    z = lax.axis_index("zh") * 4 + lax.axis_index("zl")
    same = ((j & 3) == (q & 3)) & (zl == ((q >> 2) & 3))
    return jnp.where(same, weight_value(j >> 2, position(q >> 5, z, (q >> 4) & 1)), 0.0)


def split3(x):
    hi=x.astype(BF16); r=x-hi.astype(F32); mid=r.astype(BF16); lo=(r-mid.astype(F32)).astype(BF16)
    return hi,mid,lo

def split2(x):
    hi=x.astype(BF16)
    return hi,(x-hi.astype(F32)).astype(BF16)

def onehot(ants, side, off):
    ids=ants[side:side+1, pl.ds(off,BC)]
    io=lax.broadcasted_iota(jnp.int32,(ST,BC),0)
    return jnp.where(io==ids,1.0,0.0).astype(BF16)

def gather(g3, oh, out):
    out[...]=jnp.dot(g3, jnp.concatenate([oh,oh,oh],0), preferred_element_type=F32)

def totals_body(gains, ants, m_ref, v_ref, ga, gc, x_ref, acc):
    g3=jnp.concatenate(split3(gains),1)
    acc[...]=jnp.zeros_like(acc)
    def chunk(c, _):
        off=pl.multiple_of(c*BC,BC)
        oa=onehot(ants,0,off); oc=onehot(ants,1,off)
        gather(g3,oa,ga); gather(g3,oc,gc)
        for lt in range(BC//128):
            L=slice(lt*128,lt*128+128)
            D=pl.ds(pl.multiple_of(off+lt*128,128),128)
            res=[[v_ref[r,t,:,D] for r in range(2)] for t in range(2)]
            ps=[]
            for k in range(K):
                ra=slice(k*16,k*16+16); ia=slice(128+k*16,128+k*16+16)
                ar,ai,cr,ci=ga[ra,L],ga[ia,L],gc[ra,L],gc[ia,L]
                pr=ar*cr+ai*ci; pi=ai*cr-ar*ci
                ps.append((pr,pi))
                for t in range(2):
                    mr=m_ref[0,t,k,:,D].astype(F32); mi=m_ref[1,t,k,:,D].astype(F32)
                    res[t][0]=res[t][0]-(pr*mr-pi*mi)
                    res[t][1]=res[t][1]-(pr*mi+pi*mr)
            for k in range(K):
                ra=slice(k*16,k*16+16); ia=slice(128+k*16,128+k*16+16)
                ar,ai,cr,ci=ga[ra,L],ga[ia,L],gc[ra,L],gc[ia,L]
                pr,pi=ps[k]
                dd=0.0; qr=0.0; qi=0.0
                for t in range(2):
                    mr=m_ref[0,t,k,:,D].astype(F32); mi=m_ref[1,t,k,:,D].astype(F32)
                    rr,ri=res[t]
                    qr=qr+(rr*mr+ri*mi); qi=qi+(ri*mr-rr*mi)
                    dd=dd+(mr*mr+mi*mi)
                qr=qr+pr*dd; qi=qi+pi*dd
                vals=((qr*cr-qi*ci, qr*ci+qi*cr, (cr*cr+ci*ci)*dd),
                      (qr*ar+qi*ai, qr*ai-qi*ar, (ar*ar+ai*ai)*dd))
                for s in range(2):
                    LL=slice(s*BC+lt*128,s*BC+lt*128+128)
                    for q in range(3):
                        h,l=split2(vals[s][q])
                        x_ref[q*128+k*16:q*128+k*16+16,LL]=h
                        x_ref[384+q*128+k*16:384+q*128+k*16+16,LL]=l
        oh2=jnp.concatenate([oa,oc],1)
        t=lax.dot_general(x_ref[...],oh2,NT,preferred_element_type=F32)
        acc[...]+=t[:384]+t[384:]
        return 0
    lax.fori_loop(0,BL//BC,chunk,0,unroll=2)


def unpack(jp):
    return jnp.concatenate([jp[:, :ST], jp[:, ST:]], 0)


def pack(top, bottom):
    return jnp.concatenate([top, bottom], 1)


def pack_kernel(g_ref, out):
    out[...] = pack(g_ref[0:128, :], g_ref[128:256, :])


def merge(out, fit, tmp, ab):
    tmp[...] = fit
    for r in range(4):
        at = pl.ds(r, 32, stride=4)
        out[pl.ds(r, 32, stride=10), :] = tmp[at, :]
        out[pl.ds(4 + r, 32, stride=10), :] = ab[at, :]
    left = iota((32, 128), 1) < ST
    for p in range(2):
        out[pl.ds(8 + p, 32, stride=10), :] = jnp.where(
            left, ab[pl.ds(128 + 2 * p, 32, stride=4), :], ab[pl.ds(129 + 2 * p, 32, stride=4), :])


def copies(out, value, times):
    rows = value.shape[0]
    for i in range(times):
        out[i * rows:i * rows + rows, :] = value


def first_kernel(g_ref, ants, m_ref, v_ref, ab, ga, gc, x_ref, acc):
    totals_body(g_ref[...], ants, m_ref, v_ref, ga, gc, x_ref, acc)
    inv = 1.0 / (acc[256:384, :] + RHO)
    inv = pack(inv, inv)
    ab[0:128, :] = pack(acc[0:128, :], acc[128:256, :]) * inv
    ab[128:256, :] = RHO * inv


def mm(a, b):
    return jnp.dot(a, b, precision=HIGH, preferred_element_type=F32)


def plane_kernel(recv, out):
    copies(out, mm(plane_down(), recv[...]), 4)


def summed(recv, first, count):
    total = recv[first * 12:first * 12 + 12, :]
    for i in range(1, count):
        s = (first + i) * 12
        total = total + recv[s:s + 12, :]
    return jnp.concatenate([total, jnp.zeros((4, 128), F32)], 0)


def fit_kernel(recv, ab, out, zh, tmp):
    z = mm(cube_up(), summed(recv, 0, 16))
    zh[...] = z
    merge(out, z, tmp, ab)


def coefficients(recv, t_ref, cnt):
    return averaged([summed(recv, h * 4, 4) for h in range(CL)], range(CL), t_ref, cnt)


def fit_average_kernel(recv, t_ref, cnt, ab, out, zh, tmp):
    z = mm(cube_up(), coefficients(recv, t_ref, cnt))
    zh[...] = z
    merge(out, z, tmp, ab)


def last_fit_kernel(recv, t_ref, cnt, out):
    out[...] = mm(cube_up(), coefficients(recv, t_ref, cnt))


def update_kernel(spread, got, zh, ab, part, j_out, tmp):
    left = iota((32, 128), 1) < ST
    for r in range(4):
        at = pl.ds(r, 32, stride=4)
        two = got[pl.ds(8 + r // 2, 32, stride=10), :]
        turned = jnp.concatenate([two[:, ST:], two[:, :ST]], 1)
        slope = jnp.where(left, two, turned) if r % 2 == 0 else jnp.where(left, turned, two)
        tmp[at, :] = got[pl.ds(4 + r, 32, stride=10), :] + slope * zh[at, :]
        j_out[at, :] = ab[at, :] + ab[pl.ds(128 + r, 32, stride=4), :] * got[pl.ds(r, 32, stride=10), :]
    copies(part, mm(cube_down(), tmp[...])[0:12], 16)
    for i in range(1, spread):
        j_out[i * 128:i * 128 + 128, :] = j_out[0:128, :]


def map_kernel(mine, theirs, own, ants, t_ref, cnt, kept):
    kept[...] = ants[...]
    shared = mine.shape[1]
    io = lax.broadcasted_iota(jnp.int32, (ST, shared), 0)
    eye = jnp.where(lax.broadcasted_iota(jnp.int32, (ST, ST), 0) == lax.broadcasted_iota(jnp.int32, (ST, ST), 1), 1.0, 0.0)
    zero = jnp.zeros((ST, ST), F32)
    total = jnp.zeros((8, ST), F32)
    ones = jnp.ones((8, shared), BF16)
    for h in range(CL):
        om = jnp.where(io == mine[h:h + 1, :], 1.0, 0.0).astype(BF16)
        ot = jnp.where(io == theirs[h:h + 1, :], 1.0, 0.0).astype(BF16)
        t = lax.dot_general(ot, om, NT, preferred_element_type=F32) + eye * own[h:h + 1, :]
        t_ref[h * 128:h * 128 + 128, :] = pack(jnp.concatenate([t, zero], 0), jnp.concatenate([zero, t], 0)).astype(BF16)
        total = total + lax.dot_general(ones, om, NT, preferred_element_type=F32)
    cnt[...] = 1.0 / (1.0 + pack(total, total))


def averaged(parts, clusters, t_ref, cnt):
    total = 0.0
    for x, h in zip(parts, clusters):
        t = t_ref[pl.ds(pl.multiple_of(h * 128, 128), 128), :]
        total = total + jnp.dot(jnp.concatenate(split3(x), 1), jnp.concatenate([t, t, t], 0), preferred_element_type=F32)
    return total * cnt[0:1, :]


def average_of(own, r1, r2, r3, t_ref, cnt):
    g = lax.axis_index("x")
    return averaged([own[...], r1[...], r2[...], r3[...]], [lax.rem(g + CL - s, CL) for s in range(CL)], t_ref, cnt)


def second_kernel(recv, t_ref, cnt, ants, m_ref, v_ref, ab, ga, gc, x_ref, acc):
    j1 = averaged([recv[h * 128:h * 128 + 128, :] for h in range(CL)], range(CL), t_ref, cnt)
    totals_body(unpack(j1), ants, m_ref, v_ref, ga, gc, x_ref, acc)
    inv = 1.0 / (acc[256:384, :] + RHO)
    inv = pack(inv, inv)
    ab[0:128, :] = (pack(acc[0:128, :], acc[128:256, :]) - RHO * j1) * inv
    ab[128:256, :] = (2.0 * RHO) * inv


def unpack_kernel(z_ref, out):
    out[...] = unpack(z_ref[...])


def residual_kernel(own, r1, r2, r3, t_ref, cnt, ants, m_ref, v_ref, rows, out, ga, gc):
    gains = unpack(average_of(own, r1, r2, r3, t_ref, cnt))
    rows[...] = gains
    g3 = jnp.concatenate(split3(gains), 1)
    def chunk(c,_):
        off=pl.multiple_of(c*BC,BC)
        gather(g3,onehot(ants,0,off),ga); gather(g3,onehot(ants,1,off),gc)
        for lt in range(BC//128):
            L=slice(lt*128,lt*128+128)
            D=pl.ds(pl.multiple_of(off+lt*128,128),128)
            res=[[v_ref[r,t,:,D] for r in range(2)] for t in range(2)]
            for k in range(K):
                ra=slice(k*16,k*16+16); ia=slice(128+k*16,128+k*16+16)
                ar,ai,cr,ci=ga[ra,L],ga[ia,L],gc[ra,L],gc[ia,L]
                pr=ar*cr+ai*ci; pi=ai*cr-ar*ci
                for t in range(2):
                    mr=m_ref[0,t,k,:,D].astype(F32); mi=m_ref[1,t,k,:,D].astype(F32)
                    res[t][0]=res[t][0]-(pr*mr-pi*mi)
                    res[t][1]=res[t][1]-(pr*mi+pi*mr)
            for t in range(2):
                for r in range(2): out[r,t,:,D]=res[t][r]
        return 0
    lax.fori_loop(0,BL//BC,chunk,0,unroll=2)


def kernel(body, outs, ins, scratch=(), name=None, flops=100000000, vmem=8):
    return pl.pallas_call(
        body, out_shape=outs, in_specs=[VM] * ins,
        out_specs=(VM,) * len(outs) if isinstance(outs, tuple) else VM,
        scratch_shapes=list(scratch), name=name,
        compiler_params=pltpu.CompilerParams(vmem_limit_bytes=vmem * 1048576),
        cost_estimate=pl.CostEstimate(flops=flops, bytes_accessed=1000000, transcendentals=0))


def on_device(visibilities, model, flags, antennas, correlation, gains_init):
    ants = antennas[0]
    gains = gains_init.reshape(2 * K * SI, ST)
    group = lax.axis_index("x")
    mine = lax.dynamic_index_in_dim(correlation, group, 0, keepdims=False)
    theirs = lax.dynamic_index_in_dim(correlation, group, 1, keepdims=False)
    own = jnp.broadcast_to(jnp.where(jnp.arange(CL) == group, 1.0, 0.0)[:, None], (CL, ST))
    full = SD((128, 128), F32)
    tile = pltpu.VMEM((128, 128), F32)
    exchange = functools.partial(lax.all_to_all, split_axis=0, concat_axis=0, tiled=True)
    scratch = [pltpu.VMEM((256, BC), F32), pltpu.VMEM((256, BC), F32), pltpu.VMEM((768, 2 * BC), BF16), pltpu.VMEM((384, ST), F32)]
    big = 2000000000
    wide = SD((320, 128), F32)
    pairs = SD((256, 128), F32)
    moments = SD((192, 128), F32)

    def others(j):
        return [lax.ppermute(j, "x", [(i, (i + s) % CL) for i in range(CL)]) for s in range(1, CL)]

    def swap(x, axes, *shape):
        return exchange(x.reshape(*shape, 128), axes).reshape(-1, 128)

    got = swap(kernel(pack_kernel, full, 1, name="pack")(gains), PLANE, 8, 16)
    keep = flags[0, 0] == 0
    m = jnp.where(keep[None, None], model[0][:, :, 0], jnp.zeros((), BF16)).transpose(0, 3, 1, 2, 4)
    v = jnp.where(keep[None], visibilities[0][:, 0], 0.0).transpose(0, 2, 1, 3)
    tmap, cnt, ants = kernel(map_kernel, (SD((CL * 128, 128), BF16), SD((8, 128), F32), SD((2, BL), jnp.int32)), 4, name="maps")(
        mine, theirs, own, ants)
    got, m, v, tmap, cnt, ants = lax.optimization_barrier((got, m, v, tmap, cnt, ants))
    got = swap(kernel(plane_kernel, moments, 1, name="plane")(got), ("zh", "zl"), 16, 3, 4)
    ab = kernel(first_kernel, pairs, 4, scratch, "first", big, 24)(gains, ants, m, v)

    got, ab = lax.optimization_barrier((got, ab))
    send, zh = kernel(fit_kernel, (wide, full), 2, [tile], "fit")(got, ab)
    got = swap(send, CUBE, 32, 5, 2)
    part, j1 = kernel(functools.partial(update_kernel, CL), (moments, SD((512, 128), F32)), 3, [tile], "update")(got, zh, ab)
    recv = exchange(j1, "x")
    recv, part = lax.optimization_barrier((recv, part))
    got = swap(part, ("x", "zh"), 16, 3, 4)
    ab = kernel(second_kernel, pairs, 6, scratch, "second", big, 24)(recv, tmap, cnt, ants, m, v)
    send, zh = kernel(fit_average_kernel, (wide, full), 4, [tile], "fits")(got, tmap, cnt, ab)
    got = swap(send, CUBE, 32, 5, 2)
    part, j2 = kernel(functools.partial(update_kernel, 1), (moments, full), 3, [tile], "update2")(got, zh, ab)
    got = swap(part, ("x", "zh"), 16, 3, 4)
    d2 = others(j2)
    got, *d2 = lax.optimization_barrier((got, *d2))
    rows, res = kernel(residual_kernel, (SD((256, ST), F32), SD((2, 2, SI, BL), F32)), 9, scratch[:2], "residual", big, 24)(
        j2, *d2, tmap, cnt, ants, m, v)
    z = kernel(last_fit_kernel, full, 3, name="lastfit")(got, tmap, cnt)
    zrows = kernel(unpack_kernel, SD((256, ST), F32), 1, name="unpack")(swap(z, CUBE, 32, 4))
    shape = gains_init.shape
    return rows.reshape(shape), zrows.reshape(shape), res.transpose(0, 2, 1, 3)[None, :, None]


def solution(mesh):
    split = Mesh(mesh.devices.reshape(4, 4, 4, 4, 2), ("x", "y", "zh", "zl", "c"))
    return jax.shard_map(
        on_device,
        mesh=split,
        in_specs=(
            P("x", None, CHAN, None, None, None),
            P("x", None, None, CHAN, None, None, None),
            P("x", CHAN, None, None, None),
            P("x", None, None),
            P(),
            P("x", None, None, CHAN, None, None),
        ),
        out_specs=(
            P("x", None, None, CHAN, None, None),
            P("x", None, None, CHAN, None, None),
            P("x", None, CHAN, None, None, None),
        ),
        check_vma=False,
    )
```

```python
import functools

import jax
import jax.numpy as jnp
import numpy as np
from jax import lax
from jax.experimental import pallas as pl
from jax.experimental.pallas import tpu as pltpu
from jax.sharding import Mesh, PartitionSpec as P

K, SI, ST, BL, CL, CH = 8, 16, 64, 2048, 4, 128
RHO = 128.0
F32, BF16 = jnp.float32, jnp.bfloat16
NT = (((1,), (1,)), ((), ()))
HIGH = lax.Precision.HIGHEST
BC = 512
VM = pl.BlockSpec(memory_space=pltpu.VMEM)
SD = jax.ShapeDtypeStruct
CUBE = ("y", "c", "zl")
PLANE = ("y", "c")
CHAN = ("y", "zh", "zl", "c")


def inverse_gram():
    f = np.arange(CH, dtype=np.float64)
    x = (2 * f + 1) / CH - 1
    basis = np.stack([np.ones_like(x), x, 1.5 * x * x - 0.5], axis=1)
    return np.linalg.inv(basis.T @ basis)


GINV = inverse_gram()


def iota(shape, dim):
    return lax.broadcasted_iota(jnp.int32, shape, dim)


def position(y, z, c):
    return (2 * (y * 32 + z * 2 + c) + 1).astype(F32) * (1.0 / CH) - 1.0


def basis_value(n, x):
    return jnp.where(n == 0, 1.0, jnp.where(n == 1, x, jnp.where(n == 2, 1.5 * x * x - 0.5, 0.0)))


def weight_value(n, x):
    second = 1.5 * x * x - 0.5
    rows = [float(g[0]) + float(g[1]) * x + float(g[2]) * second for g in GINV]
    return jnp.where(n == 0, rows[0], jnp.where(n == 1, rows[1], jnp.where(n == 2, rows[2], 0.0)))


def cube_entry(value, j, q):
    x = position(q >> 5, lax.axis_index("zh") * 4 + ((q >> 2) & 3), (q >> 4) & 1)
    return jnp.where((j & 3) == (q & 3), value(j >> 2, x), 0.0)


def cube_down():
    return cube_entry(weight_value, iota((16, 128), 0), iota((16, 128), 1))


def cube_up():
    return cube_entry(basis_value, iota((128, 16), 1), iota((128, 16), 0))


def plane_down():
    j, q = iota((48, 128), 0), iota((48, 128), 1)
    zl = (j * 43) >> 9
    j = j - zl * 12
    z = lax.axis_index("zh") * 4 + lax.axis_index("zl")
    same = ((j & 3) == (q & 3)) & (zl == ((q >> 2) & 3))
    return jnp.where(same, weight_value(j >> 2, position(q >> 5, z, (q >> 4) & 1)), 0.0)


def split3(x):
    hi=x.astype(BF16); r=x-hi.astype(F32); mid=r.astype(BF16); lo=(r-mid.astype(F32)).astype(BF16)
    return hi,mid,lo


def split2(x):
    hi=x.astype(BF16)
    return hi,(x-hi.astype(F32)).astype(BF16)


def onehot(ants, side, off):
    ids=ants[side:side+1, pl.ds(off,BC)]
    io=lax.broadcasted_iota(jnp.int32,(ST,BC),0)
    return jnp.where(io==ids,1.0,0.0).astype(BF16)


def gather(g3, oh, out):
    out[...]=jnp.dot(g3, jnp.concatenate([oh,oh,oh],0), preferred_element_type=F32)


def totals_body(gains, ants, m_ref, v_ref, ga, gc, x_ref, acc):
    g3=jnp.concatenate(split3(gains),1)
    acc[...]=jnp.zeros_like(acc)
    def chunk(c, _):
        off=pl.multiple_of(c*BC,BC)
        oa=onehot(ants,0,off); oc=onehot(ants,1,off)
        gather(g3,oa,ga); gather(g3,oc,gc)
        for lt in range(BC//128):
            L=slice(lt*128,lt*128+128)
            D=pl.ds(pl.multiple_of(off+lt*128,128),128)
            res=[[v_ref[r,t,:,D] for r in range(2)] for t in range(2)]
            ps=[]
            for k in range(K):
                ra=slice(k*16,k*16+16); ia=slice(128+k*16,128+k*16+16)
                ar,ai,cr,ci=ga[ra,L],ga[ia,L],gc[ra,L],gc[ia,L]
                pr=ar*cr+ai*ci; pi=ai*cr-ar*ci
                ps.append((pr,pi))
                for t in range(2):
                    mr=m_ref[0,t,k,:,D].astype(F32); mi=m_ref[1,t,k,:,D].astype(F32)
                    res[t][0]=res[t][0]-(pr*mr-pi*mi)
                    res[t][1]=res[t][1]-(pr*mi+pi*mr)
            for k in range(K):
                ra=slice(k*16,k*16+16); ia=slice(128+k*16,128+k*16+16)
                ar,ai,cr,ci=ga[ra,L],ga[ia,L],gc[ra,L],gc[ia,L]
                pr,pi=ps[k]
                dd=0.0; qr=0.0; qi=0.0
                for t in range(2):
                    mr=m_ref[0,t,k,:,D].astype(F32); mi=m_ref[1,t,k,:,D].astype(F32)
                    rr,ri=res[t]
                    qr=qr+(rr*mr+ri*mi); qi=qi+(ri*mr-rr*mi)
                    dd=dd+(mr*mr+mi*mi)
                qr=qr+pr*dd; qi=qi+pi*dd
                vals=((qr*cr-qi*ci, qr*ci+qi*cr, (cr*cr+ci*ci)*dd),
                      (qr*ar+qi*ai, qr*ai-qi*ar, (ar*ar+ai*ai)*dd))
                for s in range(2):
                    LL=slice(s*BC+lt*128,s*BC+lt*128+128)
                    for q in range(3):
                        h,l=split2(vals[s][q])
                        x_ref[q*128+k*16:q*128+k*16+16,LL]=h
                        x_ref[384+q*128+k*16:384+q*128+k*16+16,LL]=l
        oh2=jnp.concatenate([oa,oc],1)
        t=lax.dot_general(x_ref[...],oh2,NT,preferred_element_type=F32)
        acc[...]+=t[:384]+t[384:]
        return 0
    lax.fori_loop(0,BL//BC,chunk,0,unroll=2)


def unpack(jp):
    return jnp.concatenate([jp[:, :ST], jp[:, ST:]], 0)


def pack(top, bottom):
    return jnp.concatenate([top, bottom], 1)


def pack_kernel(g_ref, out):
    out[...] = pack(g_ref[0:128, :], g_ref[128:256, :])


def merge(out, fit, tmp, ab):
    tmp[...] = fit
    for r in range(4):
        at = pl.ds(r, 32, stride=4)
        out[pl.ds(r, 32, stride=10), :] = tmp[at, :]
        out[pl.ds(4 + r, 32, stride=10), :] = ab[at, :]
    left = iota((32, 128), 1) < ST
    for p in range(2):
        out[pl.ds(8 + p, 32, stride=10), :] = jnp.where(
            left, ab[pl.ds(128 + 2 * p, 32, stride=4), :], ab[pl.ds(129 + 2 * p, 32, stride=4), :])


def copies(out, value, times):
    rows = value.shape[0]
    for i in range(times):
        out[i * rows:i * rows + rows, :] = value


def first_kernel(g_ref, ants, m_ref, v_ref, ab, ga, gc, x_ref, acc):
    totals_body(g_ref[...], ants, m_ref, v_ref, ga, gc, x_ref, acc)
    inv = 1.0 / (acc[256:384, :] + RHO)
    inv = pack(inv, inv)
    ab[0:128, :] = pack(acc[0:128, :], acc[128:256, :]) * inv
    ab[128:256, :] = RHO * inv


def mm(a, b):
    return jnp.dot(a, b, precision=HIGH, preferred_element_type=F32)


def plane_kernel(recv, out):
    copies(out, mm(plane_down(), recv[...]), 4)


def summed(recv, first, count):
    total = recv[first * 12:first * 12 + 12, :]
    for i in range(1, count):
        s = (first + i) * 12
        total = total + recv[s:s + 12, :]
    return jnp.concatenate([total, jnp.zeros((4, 128), F32)], 0)


def fit_kernel(recv, ab, out, zh, tmp):
    z = mm(cube_up(), summed(recv, 0, 16))
    zh[...] = z
    merge(out, z, tmp, ab)


def coefficients(recv, t_ref, cnt):
    return averaged([summed(recv, h * 4, 4) for h in range(CL)], range(CL), t_ref, cnt)


def fit_average_kernel(recv, t_ref, cnt, ab, out, zh, tmp):
    z = mm(cube_up(), coefficients(recv, t_ref, cnt))
    zh[...] = z
    merge(out, z, tmp, ab)


def last_fit_kernel(recv, t_ref, cnt, out):
    out[...] = mm(cube_up(), coefficients(recv, t_ref, cnt))


def update_kernel(spread, got, zh, ab, part, j_out, tmp):
    left = iota((32, 128), 1) < ST
    for r in range(4):
        at = pl.ds(r, 32, stride=4)
        two = got[pl.ds(8 + r // 2, 32, stride=10), :]
        turned = jnp.concatenate([two[:, ST:], two[:, :ST]], 1)
        slope = jnp.where(left, two, turned) if r % 2 == 0 else jnp.where(left, turned, two)
        tmp[at, :] = got[pl.ds(4 + r, 32, stride=10), :] + slope * zh[at, :]
        j_out[at, :] = ab[at, :] + ab[pl.ds(128 + r, 32, stride=4), :] * got[pl.ds(r, 32, stride=10), :]
    copies(part, mm(cube_down(), tmp[...])[0:12], 16)
    for i in range(1, spread):
        j_out[i * 128:i * 128 + 128, :] = j_out[0:128, :]


def map_kernel(mine, theirs, own, ants, t_ref, cnt, kept):
    kept[...] = ants[...]
    shared = mine.shape[1]
    io = lax.broadcasted_iota(jnp.int32, (ST, shared), 0)
    eye = jnp.where(lax.broadcasted_iota(jnp.int32, (ST, ST), 0) == lax.broadcasted_iota(jnp.int32, (ST, ST), 1), 1.0, 0.0)
    zero = jnp.zeros((ST, ST), F32)
    total = jnp.zeros((8, ST), F32)
    ones = jnp.ones((8, shared), BF16)
    for h in range(CL):
        om = jnp.where(io == mine[h:h + 1, :], 1.0, 0.0).astype(BF16)
        ot = jnp.where(io == theirs[h:h + 1, :], 1.0, 0.0).astype(BF16)
        t = lax.dot_general(ot, om, NT, preferred_element_type=F32) + eye * own[h:h + 1, :]
        t_ref[h * 128:h * 128 + 128, :] = pack(jnp.concatenate([t, zero], 0), jnp.concatenate([zero, t], 0)).astype(BF16)
        total = total + lax.dot_general(ones, om, NT, preferred_element_type=F32)
    cnt[...] = 1.0 / (1.0 + pack(total, total))


def averaged(parts, clusters, t_ref, cnt):
    total = 0.0
    for x, h in zip(parts, clusters):
        t = t_ref[pl.ds(pl.multiple_of(h * 128, 128), 128), :]
        total = total + jnp.dot(jnp.concatenate(split3(x), 1), jnp.concatenate([t, t, t], 0), preferred_element_type=F32)
    return total * cnt[0:1, :]


def average_of(own, r1, r2, r3, t_ref, cnt):
    g = lax.axis_index("x")
    return averaged([own[...], r1[...], r2[...], r3[...]], [lax.rem(g + CL - s, CL) for s in range(CL)], t_ref, cnt)


def second_kernel(recv, t_ref, cnt, ants, m_ref, v_ref, ab, ga, gc, x_ref, acc):
    j1 = averaged([recv[h * 128:h * 128 + 128, :] for h in range(CL)], range(CL), t_ref, cnt)
    totals_body(unpack(j1), ants, m_ref, v_ref, ga, gc, x_ref, acc)
    inv = 1.0 / (acc[256:384, :] + RHO)
    inv = pack(inv, inv)
    ab[0:128, :] = (pack(acc[0:128, :], acc[128:256, :]) - RHO * j1) * inv
    ab[128:256, :] = (2.0 * RHO) * inv


def gate_kernel(x_ref, out):
    out[...] = x_ref[...]


def unpack_kernel(z_ref, out):
    out[...] = unpack(z_ref[...])


def residual_kernel(own, r1, r2, r3, t_ref, cnt, ants, m_ref, v_ref, rows, out, ga, gc):
    gains = unpack(average_of(own, r1, r2, r3, t_ref, cnt))
    rows[...] = gains
    g3 = jnp.concatenate(split3(gains), 1)
    def chunk(c,_):
        off=pl.multiple_of(c*BC,BC)
        gather(g3,onehot(ants,0,off),ga); gather(g3,onehot(ants,1,off),gc)
        for lt in range(BC//128):
            L=slice(lt*128,lt*128+128)
            D=pl.ds(pl.multiple_of(off+lt*128,128),128)
            res=[[v_ref[r,t,:,D] for r in range(2)] for t in range(2)]
            for k in range(K):
                ra=slice(k*16,k*16+16); ia=slice(128+k*16,128+k*16+16)
                ar,ai,cr,ci=ga[ra,L],ga[ia,L],gc[ra,L],gc[ia,L]
                pr=ar*cr+ai*ci; pi=ai*cr-ar*ci
                for t in range(2):
                    mr=m_ref[0,t,k,:,D].astype(F32); mi=m_ref[1,t,k,:,D].astype(F32)
                    res[t][0]=res[t][0]-(pr*mr-pi*mi)
                    res[t][1]=res[t][1]-(pr*mi+pi*mr)
            for t in range(2):
                for r in range(2): out[r,t,:,D]=res[t][r]
        return 0
    lax.fori_loop(0,BL//BC,chunk,0,unroll=2)


def kernel(body, outs, ins, scratch=(), flops=100000000, vmem=8):
    return pl.pallas_call(
        body, out_shape=outs, in_specs=[VM] * ins,
        out_specs=(VM,) * len(outs) if isinstance(outs, tuple) else VM,
        scratch_shapes=list(scratch),
        compiler_params=pltpu.CompilerParams(vmem_limit_bytes=vmem * 1048576),
        cost_estimate=pl.CostEstimate(flops=flops, bytes_accessed=1000000, transcendentals=0))


def on_device(visibilities, model, flags, antennas, correlation, gains_init):
    ants = antennas[0]
    gains = gains_init.reshape(2 * K * SI, ST)
    group = lax.axis_index("x")
    mine = lax.dynamic_index_in_dim(correlation, group, 0, keepdims=False)
    theirs = lax.dynamic_index_in_dim(correlation, group, 1, keepdims=False)
    own = jnp.broadcast_to(jnp.where(jnp.arange(CL) == group, 1.0, 0.0)[:, None], (CL, ST))
    full = SD((128, 128), F32)
    tile = pltpu.VMEM((128, 128), F32)
    exchange = functools.partial(lax.all_to_all, split_axis=0, concat_axis=0, tiled=True)
    scratch = [pltpu.VMEM((256, BC), F32), pltpu.VMEM((256, BC), F32), pltpu.VMEM((768, 2 * BC), BF16), pltpu.VMEM((384, ST), F32)]
    big = 2000000000
    wide = SD((320, 128), F32)
    pairs = SD((256, 128), F32)
    moments = SD((192, 128), F32)

    def others(j):
        return [lax.ppermute(j, "x", [(i, (i + s) % CL) for i in range(CL)]) for s in range(1, CL)]

    def swap(x, axes, *shape):
        return exchange(x.reshape(*shape, 128), axes).reshape(-1, 128)

    got = swap(kernel(pack_kernel, full, 1)(gains), PLANE, 8, 16)
    keep = flags[0, 0] == 0
    m = jnp.where(keep[None, None], model[0][:, :, 0], jnp.zeros((), BF16)).transpose(0, 3, 1, 2, 4)
    v = jnp.where(keep[None], visibilities[0][:, 0], 0.0).transpose(0, 2, 1, 3)
    tmap, cnt, ants = kernel(map_kernel, (SD((CL * 128, 128), BF16), SD((8, 128), F32), SD((2, BL), jnp.int32)), 4)(
        mine, theirs, own, ants)
    got, m, v, tmap, cnt, ants = lax.optimization_barrier((got, m, v, tmap, cnt, ants))
    got = swap(kernel(plane_kernel, moments, 1)(got), ("zh", "zl"), 16, 3, 4)
    ab = kernel(first_kernel, pairs, 4, scratch, big, 24)(gains, ants, m, v)

    got, ab = lax.optimization_barrier((got, ab))
    send, zh = kernel(fit_kernel, (wide, full), 2, [tile])(got, ab)
    got = swap(send, CUBE, 32, 5, 2)
    part, j1 = kernel(functools.partial(update_kernel, CL), (moments, SD((512, 128), F32)), 3, [tile])(got, zh, ab)
    recv = exchange(j1, "x")
    recv, part = lax.optimization_barrier((recv, part))
    got = swap(part, ("x", "zh"), 16, 3, 4)
    ab = kernel(second_kernel, pairs, 6, scratch, big, 24)(recv, tmap, cnt, ants, m, v)
    send, zh = kernel(fit_average_kernel, (wide, full), 4, [tile])(got, tmap, cnt, ab)
    got = swap(send, CUBE, 32, 5, 2)
    part, j2 = kernel(functools.partial(update_kernel, 1), (moments, full), 3, [tile])(got, zh, ab)
    got = swap(part, ("x", "zh"), 16, 3, 4)
    d2 = others(j2)
    cnt2 = kernel(gate_kernel, SD((8, 128), F32), 1)(cnt)
    rows, res = kernel(residual_kernel, (SD((256, ST), F32), SD((2, 2, SI, BL), F32)), 9, scratch[:2], big, 24)(
        j2, *d2, tmap, cnt2, ants, m, v)
    z = kernel(last_fit_kernel, full, 3)(got, tmap, cnt)
    zrows = kernel(unpack_kernel, SD((256, ST), F32), 1)(swap(z, CUBE, 32, 4))
    shape = gains_init.shape
    return rows.reshape(shape), zrows.reshape(shape), res.transpose(0, 2, 1, 3)[None, :, None]


def solution(mesh):
    split = Mesh(mesh.devices.reshape(4, 4, 4, 4, 2), ("x", "y", "zh", "zl", "c"))
    return jax.shard_map(
        on_device,
        mesh=split,
        in_specs=(
            P("x", None, CHAN, None, None, None),
            P("x", None, None, CHAN, None, None, None),
            P("x", CHAN, None, None, None),
            P("x", None, None),
            P(),
            P("x", None, None, CHAN, None, None),
        ),
        out_specs=(
            P("x", None, None, CHAN, None, None),
            P("x", None, None, CHAN, None, None),
            P("x", None, CHAN, None, None, None),
        ),
        check_vma=False,
    )
```

```python
import functools

import jax
import jax.numpy as jnp
import numpy as np
from jax import lax
from jax.experimental import pallas as pl
from jax.experimental.pallas import tpu as pltpu
from jax.sharding import Mesh, PartitionSpec as P

K, SI, ST, BL, CL, CH = 8, 16, 64, 2048, 4, 128
RHO = 128.0
F32, BF16 = jnp.float32, jnp.bfloat16
NT = (((1,), (1,)), ((), ()))
HIGH = lax.Precision.HIGHEST
BC = 512
VM = pl.BlockSpec(memory_space=pltpu.VMEM)
SD = jax.ShapeDtypeStruct
CUBE = ("y", "c", "zl")
PLANE = ("y", "c")
CHAN = ("y", "zh", "zl", "c")


def inverse_gram():
    f = np.arange(CH, dtype=np.float64)
    x = (2 * f + 1) / CH - 1
    basis = np.stack([np.ones_like(x), x, 1.5 * x * x - 0.5], axis=1)
    return np.linalg.inv(basis.T @ basis)


GINV = inverse_gram()


def iota(shape, dim):
    return lax.broadcasted_iota(jnp.int32, shape, dim)


def position(y, z, c):
    return (2 * (y * 32 + z * 2 + c) + 1).astype(F32) * (1.0 / CH) - 1.0


def basis_value(n, x):
    return jnp.where(n == 0, 1.0, jnp.where(n == 1, x, jnp.where(n == 2, 1.5 * x * x - 0.5, 0.0)))


def weight_value(n, x):
    second = 1.5 * x * x - 0.5
    rows = [float(g[0]) + float(g[1]) * x + float(g[2]) * second for g in GINV]
    return jnp.where(n == 0, rows[0], jnp.where(n == 1, rows[1], jnp.where(n == 2, rows[2], 0.0)))


def cube_entry(value, j, q):
    x = position(q >> 5, lax.axis_index("zh") * 4 + ((q >> 2) & 3), (q >> 4) & 1)
    return jnp.where((j & 3) == (q & 3), value(j >> 2, x), 0.0)


def cube_down():
    return cube_entry(weight_value, iota((16, 128), 0), iota((16, 128), 1))


def cube_up():
    return cube_entry(basis_value, iota((128, 16), 1), iota((128, 16), 0))


def plane_down():
    j, q = iota((48, 128), 0), iota((48, 128), 1)
    zl = (j * 43) >> 9
    j = j - zl * 12
    z = lax.axis_index("zh") * 4 + lax.axis_index("zl")
    same = ((j & 3) == (q & 3)) & (zl == ((q >> 2) & 3))
    return jnp.where(same, weight_value(j >> 2, position(q >> 5, z, (q >> 4) & 1)), 0.0)


def split3(x):
    hi=x.astype(BF16); r=x-hi.astype(F32); mid=r.astype(BF16); lo=(r-mid.astype(F32)).astype(BF16)
    return hi,mid,lo


def split2(x):
    hi=x.astype(BF16)
    return hi,(x-hi.astype(F32)).astype(BF16)


def onehot(ants, side, off):
    ids=ants[side:side+1, pl.ds(off,BC)]
    io=lax.broadcasted_iota(jnp.int32,(ST,BC),0)
    return jnp.where(io==ids,1.0,0.0).astype(BF16)


def gather(g3, oh, out):
    out[...]=jnp.dot(g3, jnp.concatenate([oh,oh,oh],0), preferred_element_type=F32)


def totals_body(gains, ants, m_ref, v_ref, ga, gc, x_ref, acc):
    g3=jnp.concatenate(split3(gains),1)
    acc[...]=jnp.zeros_like(acc)
    def chunk(c, _):
        off=pl.multiple_of(c*BC,BC)
        oa=onehot(ants,0,off); oc=onehot(ants,1,off)
        gather(g3,oa,ga); gather(g3,oc,gc)
        for lt in range(BC//128):
            L=slice(lt*128,lt*128+128)
            D=pl.ds(pl.multiple_of(off+lt*128,128),128)
            res=[[v_ref[r,t,:,D] for r in range(2)] for t in range(2)]
            ps=[]
            for k in range(K):
                ra=slice(k*16,k*16+16); ia=slice(128+k*16,128+k*16+16)
                ar,ai,cr,ci=ga[ra,L],ga[ia,L],gc[ra,L],gc[ia,L]
                pr=ar*cr+ai*ci; pi=ai*cr-ar*ci
                ps.append((pr,pi))
                for t in range(2):
                    mr=m_ref[0,t,k,:,D].astype(F32); mi=m_ref[1,t,k,:,D].astype(F32)
                    res[t][0]=res[t][0]-(pr*mr-pi*mi)
                    res[t][1]=res[t][1]-(pr*mi+pi*mr)
            for k in range(K):
                ra=slice(k*16,k*16+16); ia=slice(128+k*16,128+k*16+16)
                ar,ai,cr,ci=ga[ra,L],ga[ia,L],gc[ra,L],gc[ia,L]
                pr,pi=ps[k]
                dd=0.0; qr=0.0; qi=0.0
                for t in range(2):
                    mr=m_ref[0,t,k,:,D].astype(F32); mi=m_ref[1,t,k,:,D].astype(F32)
                    rr,ri=res[t]
                    qr=qr+(rr*mr+ri*mi); qi=qi+(ri*mr-rr*mi)
                    dd=dd+(mr*mr+mi*mi)
                qr=qr+pr*dd; qi=qi+pi*dd
                vals=((qr*cr-qi*ci, qr*ci+qi*cr, (cr*cr+ci*ci)*dd),
                      (qr*ar+qi*ai, qr*ai-qi*ar, (ar*ar+ai*ai)*dd))
                for s in range(2):
                    LL=slice(s*BC+lt*128,s*BC+lt*128+128)
                    for q in range(3):
                        h,l=split2(vals[s][q])
                        x_ref[q*128+k*16:q*128+k*16+16,LL]=h
                        x_ref[384+q*128+k*16:384+q*128+k*16+16,LL]=l
        oh2=jnp.concatenate([oa,oc],1)
        t=lax.dot_general(x_ref[...],oh2,NT,preferred_element_type=F32)
        acc[...]+=t[:384]+t[384:]
        return 0
    lax.fori_loop(0,BL//BC,chunk,0,unroll=4)


def unpack(jp):
    return jnp.concatenate([jp[:, :ST], jp[:, ST:]], 0)


def pack(top, bottom):
    return jnp.concatenate([top, bottom], 1)


def pack_kernel(g_ref, out):
    out[...] = pack(g_ref[0:128, :], g_ref[128:256, :])


def merge(out, fit, tmp, ab):
    tmp[...] = fit
    for r in range(4):
        at = pl.ds(r, 32, stride=4)
        out[pl.ds(r, 32, stride=10), :] = tmp[at, :]
        out[pl.ds(4 + r, 32, stride=10), :] = ab[at, :]
    left = iota((32, 128), 1) < ST
    for p in range(2):
        out[pl.ds(8 + p, 32, stride=10), :] = jnp.where(
            left, ab[pl.ds(128 + 2 * p, 32, stride=4), :], ab[pl.ds(129 + 2 * p, 32, stride=4), :])


def copies(out, value, times):
    rows = value.shape[0]
    for i in range(times):
        out[i * rows:i * rows + rows, :] = value


def first_kernel(g_ref, ants, m_ref, v_ref, ab, ga, gc, x_ref, acc):
    totals_body(g_ref[...], ants, m_ref, v_ref, ga, gc, x_ref, acc)
    inv = 1.0 / (acc[256:384, :] + RHO)
    inv = pack(inv, inv)
    ab[0:128, :] = pack(acc[0:128, :], acc[128:256, :]) * inv
    ab[128:256, :] = RHO * inv


def mm(a, b):
    return jnp.dot(a, b, precision=HIGH, preferred_element_type=F32)


def plane_kernel(recv, out):
    copies(out, mm(plane_down(), recv[...]), 4)


def summed(recv, first, count):
    total = recv[first * 12:first * 12 + 12, :]
    for i in range(1, count):
        s = (first + i) * 12
        total = total + recv[s:s + 12, :]
    return jnp.concatenate([total, jnp.zeros((4, 128), F32)], 0)


def fit_kernel(count, recv, ab, out, zh, tmp):
    z = mm(cube_up(), summed(recv, 0, count))
    zh[...] = z
    merge(out, z, tmp, ab)


def coefficients(recv, t_ref, cnt):
    return averaged([summed(recv, h * 4, 4) for h in range(CL)], range(CL), t_ref, cnt)


def last_fit_kernel(recv, t_ref, cnt, out):
    out[...] = mm(cube_up(), coefficients(recv, t_ref, cnt))


def stepped(got, zh, ab, tmp, j_out):
    left = iota((32, 128), 1) < ST
    for r in range(4):
        at = pl.ds(r, 32, stride=4)
        two = got[pl.ds(8 + r // 2, 32, stride=10), :]
        turned = jnp.concatenate([two[:, ST:], two[:, :ST]], 1)
        slope = jnp.where(left, two, turned) if r % 2 == 0 else jnp.where(left, turned, two)
        tmp[at, :] = got[pl.ds(4 + r, 32, stride=10), :] + slope * zh[at, :]
        j_out[at, :] = ab[at, :] + ab[pl.ds(128 + r, 32, stride=4), :] * got[pl.ds(r, 32, stride=10), :]
    return mm(cube_down(), tmp[...])


def update_kernel(got, zh, ab, out, tmp, own):
    part = stepped(got, zh, ab, tmp, own)
    for h in range(CL):
        out[h * 144:h * 144 + 128, :] = own[...]
        out[h * 144 + 128:h * 144 + 144, :] = part


def second_update_kernel(got, zh, ab, part, j_out, tmp):
    copies(part, stepped(got, zh, ab, tmp, j_out)[0:12], 16)


def meet_kernel(recv, t_ref, cnt, out):
    copies(out, averaged([recv[h * 144 + 128:h * 144 + 144, :] for h in range(CL)], range(CL), t_ref, cnt)[0:12], 4)


def map_kernel(mine, theirs, own, ants, t_ref, cnt, kept):
    kept[...] = ants[...]
    shared = mine.shape[1]
    io = lax.broadcasted_iota(jnp.int32, (ST, shared), 0)
    eye = jnp.where(lax.broadcasted_iota(jnp.int32, (ST, ST), 0) == lax.broadcasted_iota(jnp.int32, (ST, ST), 1), 1.0, 0.0)
    zero = jnp.zeros((ST, ST), F32)
    total = jnp.zeros((8, ST), F32)
    ones = jnp.ones((8, shared), BF16)
    for h in range(CL):
        om = jnp.where(io == mine[h:h + 1, :], 1.0, 0.0).astype(BF16)
        ot = jnp.where(io == theirs[h:h + 1, :], 1.0, 0.0).astype(BF16)
        t = lax.dot_general(ot, om, NT, preferred_element_type=F32) + eye * own[h:h + 1, :]
        t_ref[h * 128:h * 128 + 128, :] = pack(jnp.concatenate([t, zero], 0), jnp.concatenate([zero, t], 0)).astype(BF16)
        total = total + lax.dot_general(ones, om, NT, preferred_element_type=F32)
    cnt[...] = 1.0 / (1.0 + pack(total, total))


def averaged(parts, clusters, t_ref, cnt):
    total = 0.0
    for x, h in zip(parts, clusters):
        t = t_ref[pl.ds(pl.multiple_of(h * 128, 128), 128), :]
        total = total + jnp.dot(jnp.concatenate(split3(x), 1), jnp.concatenate([t, t, t], 0), preferred_element_type=F32)
    return total * cnt[0:1, :]


def average_of(own, r1, r2, r3, t_ref, cnt):
    g = lax.axis_index("x")
    return averaged([own[...], r1[...], r2[...], r3[...]], [lax.rem(g + CL - s, CL) for s in range(CL)], t_ref, cnt)


def second_kernel(recv, t_ref, cnt, ants, m_ref, v_ref, ab, ga, gc, x_ref, acc):
    j1 = averaged([recv[h * 144:h * 144 + 128, :] for h in range(CL)], range(CL), t_ref, cnt)
    totals_body(unpack(j1), ants, m_ref, v_ref, ga, gc, x_ref, acc)
    inv = 1.0 / (acc[256:384, :] + RHO)
    inv = pack(inv, inv)
    ab[0:128, :] = (pack(acc[0:128, :], acc[128:256, :]) - RHO * j1) * inv
    ab[128:256, :] = (2.0 * RHO) * inv


def gate_kernel(x_ref, out):
    out[...] = x_ref[...]


def unpack_kernel(z_ref, out):
    out[...] = unpack(z_ref[...])


def residual_kernel(own, r1, r2, r3, t_ref, cnt, ants, m_ref, v_ref, rows, out, ga, gc):
    gains = unpack(average_of(own, r1, r2, r3, t_ref, cnt))
    rows[...] = gains
    g3 = jnp.concatenate(split3(gains), 1)
    def chunk(c,_):
        off=pl.multiple_of(c*BC,BC)
        gather(g3,onehot(ants,0,off),ga); gather(g3,onehot(ants,1,off),gc)
        for lt in range(BC//128):
            L=slice(lt*128,lt*128+128)
            D=pl.ds(pl.multiple_of(off+lt*128,128),128)
            res=[[v_ref[r,t,:,D] for r in range(2)] for t in range(2)]
            for k in range(K):
                ra=slice(k*16,k*16+16); ia=slice(128+k*16,128+k*16+16)
                ar,ai,cr,ci=ga[ra,L],ga[ia,L],gc[ra,L],gc[ia,L]
                pr=ar*cr+ai*ci; pi=ai*cr-ar*ci
                for t in range(2):
                    mr=m_ref[0,t,k,:,D].astype(F32); mi=m_ref[1,t,k,:,D].astype(F32)
                    res[t][0]=res[t][0]-(pr*mr-pi*mi)
                    res[t][1]=res[t][1]-(pr*mi+pi*mr)
            for t in range(2):
                for r in range(2): out[r,t,:,D]=res[t][r]
        return 0
    lax.fori_loop(0,BL//BC,chunk,0,unroll=4)


def kernel(body, outs, ins, scratch=(), flops=100000000, vmem=8):
    return pl.pallas_call(
        body, out_shape=outs, in_specs=[VM] * ins,
        out_specs=(VM,) * len(outs) if isinstance(outs, tuple) else VM,
        scratch_shapes=list(scratch),
        compiler_params=pltpu.CompilerParams(vmem_limit_bytes=vmem * 1048576),
        cost_estimate=pl.CostEstimate(flops=flops, bytes_accessed=1000000, transcendentals=0))


def on_device(visibilities, model, flags, antennas, correlation, gains_init):
    ants = antennas[0]
    gains = gains_init.reshape(2 * K * SI, ST)
    group = lax.axis_index("x")
    mine = lax.dynamic_index_in_dim(correlation, group, 0, keepdims=False)
    theirs = lax.dynamic_index_in_dim(correlation, group, 1, keepdims=False)
    own = jnp.broadcast_to(jnp.where(jnp.arange(CL) == group, 1.0, 0.0)[:, None], (CL, ST))
    full = SD((128, 128), F32)
    tile = pltpu.VMEM((128, 128), F32)
    exchange = functools.partial(lax.all_to_all, split_axis=0, concat_axis=0, tiled=True)
    scratch = [pltpu.VMEM((256, BC), F32), pltpu.VMEM((256, BC), F32), pltpu.VMEM((768, 2 * BC), BF16), pltpu.VMEM((384, ST), F32)]
    big = 2000000000
    wide = SD((320, 128), F32)
    pairs = SD((256, 128), F32)
    moments = SD((192, 128), F32)

    def others(j):
        return [lax.ppermute(j, "x", [(i, (i + s) % CL) for i in range(CL)]) for s in range(1, CL)]

    def swap(x, axes, *shape):
        return exchange(x.reshape(*shape, 128), axes).reshape(-1, 128)

    got = swap(kernel(pack_kernel, full, 1)(gains), PLANE, 8, 16)
    keep = flags[0, 0] == 0
    m = jnp.where(keep[None, None], model[0][:, :, 0], jnp.zeros((), BF16)).transpose(0, 3, 1, 2, 4)
    v = jnp.where(keep[None], visibilities[0][:, 0], 0.0).transpose(0, 2, 1, 3)
    tmap, cnt, ants = kernel(map_kernel, (SD((CL * 128, 128), BF16), SD((8, 128), F32), SD((2, BL), jnp.int32)), 4)(
        mine, theirs, own, ants)
    got, m, v, tmap, cnt, ants = lax.optimization_barrier((got, m, v, tmap, cnt, ants))
    got = swap(kernel(plane_kernel, moments, 1)(got), ("zh", "zl"), 16, 3, 4)
    ab = kernel(first_kernel, pairs, 4, scratch, big, 24)(gains, ants, m, v)

    got, ab = lax.optimization_barrier((got, ab))
    send, zh = kernel(functools.partial(fit_kernel, 16), (wide, full), 2, [tile])(got, ab)
    got = swap(send, CUBE, 32, 5, 2)
    recv = exchange(kernel(update_kernel, SD((576, 128), F32), 3, [tile, tile])(got, zh, ab), "x")
    part = kernel(meet_kernel, SD((48, 128), F32), 3)(recv, tmap, cnt)
    got = swap(part, "zh", 4, 3, 4)
    ab = kernel(second_kernel, pairs, 6, scratch, big, 24)(recv, tmap, cnt, ants, m, v)
    send, zh = kernel(functools.partial(fit_kernel, 4), (wide, full), 2, [tile])(got, ab)
    got = swap(send, CUBE, 32, 5, 2)
    part, j2 = kernel(second_update_kernel, (moments, full), 3, [tile])(got, zh, ab)
    got = swap(part, ("x", "zh"), 16, 3, 4)
    d2 = others(j2)
    cnt2 = kernel(gate_kernel, SD((8, 128), F32), 1)(cnt)
    rows, res = kernel(residual_kernel, (SD((256, ST), F32), SD((2, 2, SI, BL), F32)), 9, scratch[:2], big, 24)(
        j2, *d2, tmap, cnt2, ants, m, v)
    z = kernel(last_fit_kernel, full, 3)(got, tmap, cnt)
    zrows = kernel(unpack_kernel, SD((256, ST), F32), 1)(swap(z, CUBE, 32, 4))
    shape = gains_init.shape
    return rows.reshape(shape), zrows.reshape(shape), res.transpose(0, 2, 1, 3)[None, :, None]


def solution(mesh):
    split = Mesh(mesh.devices.reshape(4, 4, 4, 4, 2), ("x", "y", "zh", "zl", "c"))
    return jax.shard_map(
        on_device,
        mesh=split,
        in_specs=(
            P("x", None, CHAN, None, None, None),
            P("x", None, None, CHAN, None, None, None),
            P("x", CHAN, None, None, None),
            P("x", None, None),
            P(),
            P("x", None, None, CHAN, None, None),
        ),
        out_specs=(
            P("x", None, None, CHAN, None, None),
            P("x", None, None, CHAN, None, None),
            P("x", None, CHAN, None, None, None),
        ),
        check_vma=False,
    )
```

```python
import functools

import jax
import jax.numpy as jnp
import numpy as np
from jax import lax
from jax.experimental import pallas as pl
from jax.experimental.pallas import tpu as pltpu
from jax.sharding import Mesh, PartitionSpec as P

K, SI, ST, BL, CL, CH = 8, 16, 64, 2048, 4, 128
RHO = 128.0
F32, BF16 = jnp.float32, jnp.bfloat16
NT = (((1,), (1,)), ((), ()))
BC = 512
VM = pl.BlockSpec(memory_space=pltpu.VMEM)
SD = jax.ShapeDtypeStruct
CUBE = ("y", "c", "zl")
PLANE = ("y", "c")
CHAN = ("y", "zh", "zl", "c")


def inverse_gram():
    f = np.arange(CH, dtype=np.float64)
    x = (2 * f + 1) / CH - 1
    basis = np.stack([np.ones_like(x), x, 1.5 * x * x - 0.5], axis=1)
    return np.linalg.inv(basis.T @ basis)


GINV = inverse_gram()


def iota(shape, dim):
    return lax.broadcasted_iota(jnp.int32, shape, dim)


def position(y, z, c):
    return (2 * (y * 32 + z * 2 + c) + 1).astype(F32) * (1.0 / CH) - 1.0


def basis_value(n, x):
    return jnp.where(n == 0, 1.0, jnp.where(n == 1, x, jnp.where(n == 2, 1.5 * x * x - 0.5, 0.0)))


def weight_value(n, x):
    second = 1.5 * x * x - 0.5
    rows = [float(g[0]) + float(g[1]) * x + float(g[2]) * second for g in GINV]
    return jnp.where(n == 0, rows[0], jnp.where(n == 1, rows[1], jnp.where(n == 2, rows[2], 0.0)))


def cube_entry(value, j, q):
    x = position(q >> 5, lax.axis_index("zh") * 4 + ((q >> 2) & 3), (q >> 4) & 1)
    return jnp.where((j & 3) == (q & 3), value(j >> 2, x), 0.0)


def cube_down():
    return cube_entry(weight_value, iota((16, 128), 0), iota((16, 128), 1))


def plane_down():
    j, q = iota((48, 128), 0), iota((48, 128), 1)
    zl = (j * 43) >> 9
    j = j - zl * 12
    z = lax.axis_index("zh") * 4 + lax.axis_index("zl")
    same = ((j & 3) == (q & 3)) & (zl == ((q >> 2) & 3))
    return jnp.where(same, weight_value(j >> 2, position(q >> 5, z, (q >> 4) & 1)), 0.0)


def split3(x):
    hi=x.astype(BF16); r=x-hi.astype(F32); mid=r.astype(BF16); lo=(r-mid.astype(F32)).astype(BF16)
    return hi,mid,lo


def split2(x):
    hi=x.astype(BF16)
    return hi,(x-hi.astype(F32)).astype(BF16)


def onehot(ants, side, off):
    ids=ants[side:side+1, pl.ds(off,BC)]
    io=lax.broadcasted_iota(jnp.int32,(ST,BC),0)
    return jnp.where(io==ids,1.0,0.0).astype(BF16)


def gather(g3, oh, out):
    out[...]=jnp.dot(g3, jnp.concatenate([oh,oh,oh],0), preferred_element_type=F32)


def totals_body(gains, ants, m_ref, v_ref, ga2, gc2, x2, acc):
    g3=jnp.concatenate(split3(gains),1)
    acc[...]=jnp.zeros_like(acc)
    def chunk(c):
        off=c*BC; ga=ga2.at[c%2]; gc=gc2.at[c%2]; x_ref=x2.at[c%2]
        oa=onehot(ants,0,off); oc=onehot(ants,1,off)
        if c==0:
            gather(g3,oa,ga); gather(g3,oc,gc)
        if c+1<BL//BC:
            gather(g3,onehot(ants,0,off+BC),ga2.at[(c+1)%2]); gather(g3,onehot(ants,1,off+BC),gc2.at[(c+1)%2])
        for lt in range(BC//128):
            L=slice(lt*128,lt*128+128)
            D=slice(off+lt*128,off+lt*128+128)
            res=[[v_ref[r,t,:,D] for r in range(2)] for t in range(2)]
            for k in range(K):
                ra=slice(k*16,k*16+16); ia=slice(128+k*16,128+k*16+16)
                ar,ai,cr,ci=ga[ra,L],ga[ia,L],gc[ra,L],gc[ia,L]
                pr=ar*cr+ai*ci; pi=ai*cr-ar*ci
                for t in range(2):
                    mr=m_ref[0,t,k,:,D].astype(F32); mi=m_ref[1,t,k,:,D].astype(F32)
                    res[t][0]=res[t][0]-(pr*mr-pi*mi)
                    res[t][1]=res[t][1]-(pr*mi+pi*mr)
            for k in range(K):
                ra=slice(k*16,k*16+16); ia=slice(128+k*16,128+k*16+16)
                ar,ai,cr,ci=ga[ra,L],ga[ia,L],gc[ra,L],gc[ia,L]
                dd=0.0; qr=0.0; qi=0.0
                for t in range(2):
                    mr=m_ref[0,t,k,:,D].astype(F32); mi=m_ref[1,t,k,:,D].astype(F32)
                    rr,ri=res[t]
                    qr=qr+(rr*mr+ri*mi); qi=qi+(ri*mr-rr*mi)
                    dd=dd+(mr*mr+mi*mi)
                vals=((qr*cr-qi*ci, qr*ci+qi*cr, (cr*cr+ci*ci)*dd),
                      (qr*ar+qi*ai, qr*ai-qi*ar, (ar*ar+ai*ai)*dd))
                for s in range(2):
                    LL=slice(s*BC+lt*128,s*BC+lt*128+128)
                    for q in range(3):
                        h,l=split2(vals[s][q])
                        x_ref[q*128+k*16:q*128+k*16+16,LL]=h
                        x_ref[384+q*128+k*16:384+q*128+k*16+16,LL]=l
        oh2=jnp.concatenate([oa,oc],1)
        t=lax.dot_general(x_ref[...],oh2,NT,preferred_element_type=F32)
        acc[...]+=t[:384]+t[384:]
        return 0
    for c in range(BL//BC): chunk(c)
    den=acc[256:384,:]
    acc[0:256,:]=acc[0:256,:]+gains*jnp.concatenate([den,den],0)


def unpack(jp):
    return jnp.concatenate([jp[:, :ST], jp[:, ST:]], 0)


def pack(top, bottom):
    return jnp.concatenate([top, bottom], 1)


def pack_kernel(g_ref, out):
    out[...] = pack(g_ref[0:128, :], g_ref[128:256, :])


def merge(out, fit, tmp, ab):
    tmp[...] = fit
    for r in range(4):
        at = pl.ds(r, 32, stride=4)
        out[pl.ds(r, 32, stride=10), :] = tmp[at, :]
        out[pl.ds(4 + r, 32, stride=10), :] = ab[at, :]
    left = iota((32, 128), 1) < ST
    for p in range(2):
        out[pl.ds(8 + p, 32, stride=10), :] = jnp.where(
            left, ab[pl.ds(128 + 2 * p, 32, stride=4), :], ab[pl.ds(129 + 2 * p, 32, stride=4), :])


def copies(out, value, times):
    rows = value.shape[0]
    for i in range(times):
        out[i * rows:i * rows + rows, :] = value


def first_kernel(g_ref, ants, m_ref, v_ref, ab, ga, gc, x_ref, acc):
    totals_body(g_ref[...], ants, m_ref, v_ref, ga, gc, x_ref, acc)
    inv = 1.0 / (acc[256:384, :] + RHO)
    inv = pack(inv, inv)
    ab[0:128, :] = pack(acc[0:128, :], acc[128:256, :]) * inv
    ab[128:256, :] = RHO * inv


def mm(a, b):
    a0, a1, a2 = split3(a)
    b0, b1, b2 = split3(b)
    return jnp.dot(jnp.concatenate([a0, a0, a0, a1, a1, a2], 1), jnp.concatenate([b0, b1, b2, b0, b1, b0], 0),
                   preferred_element_type=F32)


def expand(coef):
    j, q = iota((128, 96), 1), iota((128, 96), 0)
    piece = j >> 4
    whole = cube_entry(basis_value, j & 15, q)
    high = whole.astype(BF16).astype(F32)
    rest = whole - high
    middle = rest.astype(BF16).astype(F32)
    up = jnp.where(piece < 3, high, jnp.where(piece < 5, middle, rest - middle)).astype(BF16)
    c0, c1, c2 = split3(coef)
    return jnp.dot(up, jnp.concatenate([c0, c1, c2, c0, c1, c0], 0), preferred_element_type=F32)


def plane_kernel(recv, out):
    copies(out, mm(plane_down(), recv[...]), 4)


def summed(recv, first, count):
    total = recv[first * 12:first * 12 + 12, :]
    for i in range(1, count):
        s = (first + i) * 12
        total = total + recv[s:s + 12, :]
    return jnp.concatenate([total, jnp.zeros((4, 128), F32)], 0)


def fit_kernel(count, recv, ab, out, zh, tmp):
    z = expand(summed(recv, 0, count))
    zh[...] = z
    merge(out, z, tmp, ab)


def coefficients(recv, t_ref, cnt):
    return averaged([summed(recv, h * 4, 4) for h in range(CL)], range(CL), t_ref, cnt)


def last_fit_kernel(recv, t_ref, cnt, out):
    out[...] = expand(coefficients(recv, t_ref, cnt))


def stepped(got, zh, ab, tmp, j_out):
    left = iota((32, 128), 1) < ST
    for r in range(4):
        at = pl.ds(r, 32, stride=4)
        two = got[pl.ds(8 + r // 2, 32, stride=10), :]
        turned = jnp.concatenate([two[:, ST:], two[:, :ST]], 1)
        slope = jnp.where(left, two, turned) if r % 2 == 0 else jnp.where(left, turned, two)
        tmp[at, :] = got[pl.ds(4 + r, 32, stride=10), :] + slope * zh[at, :]
        j_out[at, :] = ab[at, :] + ab[pl.ds(128 + r, 32, stride=4), :] * got[pl.ds(r, 32, stride=10), :]
    return mm(cube_down(), tmp[...])


def update_kernel(got, zh, ab, out, tmp, own):
    part = stepped(got, zh, ab, tmp, own)
    for h in range(CL):
        out[h * 144:h * 144 + 128, :] = own[...]
        out[h * 144 + 128:h * 144 + 144, :] = part


def second_update_kernel(got, zh, ab, part, j_out, tmp):
    copies(part, stepped(got, zh, ab, tmp, j_out)[0:12], 16)


def meet_kernel(recv, t_ref, cnt, out):
    copies(out, averaged([recv[h * 144 + 128:h * 144 + 144, :] for h in range(CL)], range(CL), t_ref, cnt)[0:12], 4)


def map_kernel(mine, theirs, own, ants, t_ref, cnt, kept):
    kept[...] = ants[...]
    shared = mine.shape[1]
    io = lax.broadcasted_iota(jnp.int32, (ST, shared), 0)
    eye = jnp.where(lax.broadcasted_iota(jnp.int32, (ST, ST), 0) == lax.broadcasted_iota(jnp.int32, (ST, ST), 1), 1.0, 0.0)
    zero = jnp.zeros((ST, ST), F32)
    total = jnp.zeros((8, ST), F32)
    ones = jnp.ones((8, shared), BF16)
    for h in range(CL):
        om = jnp.where(io == mine[h:h + 1, :], 1.0, 0.0).astype(BF16)
        ot = jnp.where(io == theirs[h:h + 1, :], 1.0, 0.0).astype(BF16)
        t = lax.dot_general(ot, om, NT, preferred_element_type=F32) + eye * own[h:h + 1, :]
        t_ref[h * 128:h * 128 + 128, :] = pack(jnp.concatenate([t, zero], 0), jnp.concatenate([zero, t], 0)).astype(BF16)
        total = total + lax.dot_general(ones, om, NT, preferred_element_type=F32)
    cnt[...] = 1.0 / (1.0 + pack(total, total))


def averaged(parts, clusters, t_ref, cnt):
    total = 0.0
    for x, h in zip(parts, clusters):
        t = t_ref[pl.ds(pl.multiple_of(h * 128, 128), 128), :]
        total = total + jnp.dot(jnp.concatenate(split3(x), 1), jnp.concatenate([t, t, t], 0), preferred_element_type=F32)
    return total * cnt[0:1, :]


def average_of(own, r1, r2, r3, t_ref, cnt):
    g = lax.axis_index("x")
    return averaged([own[...], r1[...], r2[...], r3[...]], [lax.rem(g + CL - s, CL) for s in range(CL)], t_ref, cnt)


def second_kernel(recv, t_ref, cnt, ants, m_ref, v_ref, ab, ga, gc, x_ref, acc):
    j1 = averaged([recv[h * 144:h * 144 + 128, :] for h in range(CL)], range(CL), t_ref, cnt)
    totals_body(unpack(j1), ants, m_ref, v_ref, ga, gc, x_ref, acc)
    inv = 1.0 / (acc[256:384, :] + RHO)
    inv = pack(inv, inv)
    ab[0:128, :] = (pack(acc[0:128, :], acc[128:256, :]) - RHO * j1) * inv
    ab[128:256, :] = (2.0 * RHO) * inv


def gate_kernel(x_ref, out):
    out[...] = x_ref[...]


def unpack_kernel(z_ref, out):
    out[...] = unpack(z_ref[...])


def residual_kernel(own, r1, r2, r3, t_ref, cnt, ants, m_ref, v_ref, rows, out, ga, gc):
    gains = unpack(average_of(own, r1, r2, r3, t_ref, cnt))
    rows[...] = gains
    g3 = jnp.concatenate(split3(gains), 1)
    def chunk(c,_):
        off=pl.multiple_of(c*BC,BC)
        gather(g3,onehot(ants,0,off),ga); gather(g3,onehot(ants,1,off),gc)
        for lt in range(BC//128):
            L=slice(lt*128,lt*128+128)
            D=pl.ds(pl.multiple_of(off+lt*128,128),128)
            res=[[v_ref[r,t,:,D] for r in range(2)] for t in range(2)]
            for k in range(K):
                ra=slice(k*16,k*16+16); ia=slice(128+k*16,128+k*16+16)
                ar,ai,cr,ci=ga[ra,L],ga[ia,L],gc[ra,L],gc[ia,L]
                pr=ar*cr+ai*ci; pi=ai*cr-ar*ci
                for t in range(2):
                    mr=m_ref[0,t,k,:,D].astype(F32); mi=m_ref[1,t,k,:,D].astype(F32)
                    res[t][0]=res[t][0]-(pr*mr-pi*mi)
                    res[t][1]=res[t][1]-(pr*mi+pi*mr)
            for t in range(2):
                for r in range(2): out[r,t,:,D]=res[t][r]
        return 0
    lax.fori_loop(0,BL//BC,chunk,0,unroll=4)


def kernel(body, outs, ins, scratch=(), flops=100000000, vmem=8, moved=1000000):
    return pl.pallas_call(
        body, out_shape=outs, in_specs=[VM] * ins,
        out_specs=(VM,) * len(outs) if isinstance(outs, tuple) else VM,
        scratch_shapes=list(scratch),
        compiler_params=pltpu.CompilerParams(vmem_limit_bytes=vmem * 1048576),
        cost_estimate=pl.CostEstimate(flops=flops, bytes_accessed=moved, transcendentals=0))


def on_device(visibilities, model, flags, antennas, correlation, gains_init):
    ants = antennas[0]
    gains = gains_init.reshape(2 * K * SI, ST)
    group = lax.axis_index("x")
    mine = lax.dynamic_index_in_dim(correlation, group, 0, keepdims=False)
    theirs = lax.dynamic_index_in_dim(correlation, group, 1, keepdims=False)
    own = jnp.broadcast_to(jnp.where(jnp.arange(CL) == group, 1.0, 0.0)[:, None], (CL, ST))
    full = SD((128, 128), F32)
    tile = pltpu.VMEM((128, 128), F32)
    exchange = functools.partial(lax.all_to_all, split_axis=0, concat_axis=0, tiled=True)
    scratch = [pltpu.VMEM((2, 256, BC), F32), pltpu.VMEM((2, 256, BC), F32), pltpu.VMEM((2, 768, 2 * BC), BF16), pltpu.VMEM((384, ST), F32)]
    spread = [pltpu.VMEM((256, BC), F32), pltpu.VMEM((256, BC), F32)]
    big = 2000000000
    wide = SD((320, 128), F32)
    pairs = SD((256, 128), F32)
    moments = SD((192, 128), F32)

    def other(j, s):
        return lax.ppermute(j, "x", [(i, (i + s) % CL) for i in range(CL)])

    def swap(x, axes, *shape):
        return exchange(x.reshape(*shape, 128), axes).reshape(-1, 128)

    got = swap(kernel(pack_kernel, full, 1, flops=20000000000, moved=20000000)(gains), PLANE, 8, 16)
    keep = flags[0, 0] == 0
    m = jnp.where(keep[None, None], model[0][:, :, 0], jnp.zeros((), BF16)).transpose(0, 3, 1, 2, 4)
    v = jnp.where(keep[None], visibilities[0][:, 0], 0.0).transpose(0, 2, 1, 3)
    tmap, cnt, ants = kernel(map_kernel, (SD((CL * 128, 128), BF16), SD((8, 128), F32), SD((2, BL), jnp.int32)), 4)(
        mine, theirs, own, ants)
    got, m, v, tmap, cnt, ants = lax.optimization_barrier((got, m, v, tmap, cnt, ants))
    got = swap(kernel(plane_kernel, moments, 1)(got), ("zh", "zl"), 16, 3, 4)
    ab = kernel(first_kernel, pairs, 4, scratch, big, 24)(gains, ants, m, v)

    got, ab = lax.optimization_barrier((got, ab))
    send, zh = kernel(functools.partial(fit_kernel, 16), (wide, full), 2, [tile])(got, ab)
    got = swap(send, CUBE, 32, 5, 2)
    recv = exchange(kernel(update_kernel, SD((576, 128), F32), 3, [tile, tile])(got, zh, ab), "x")
    part = kernel(meet_kernel, SD((48, 128), F32), 3)(recv, tmap, cnt)
    got = swap(part, "zh", 4, 3, 4)
    ab = kernel(second_kernel, pairs, 6, scratch, big, 24)(recv, tmap, cnt, ants, m, v)
    send, zh = kernel(functools.partial(fit_kernel, 4), (wide, full), 2, [tile])(got, ab)
    got = swap(send, CUBE, 32, 5, 2)
    part, j2 = kernel(second_update_kernel, (moments, full), 3, [tile])(got, zh, ab)
    got = swap(part, ("x", "zh"), 16, 3, 4)
    r2, r3 = other(j2, 2), other(j2, 3)
    cnt2 = kernel(gate_kernel, SD((8, 128), F32), 1)(cnt)
    z = kernel(last_fit_kernel, full, 3)(got, tmap, cnt)
    z = swap(z, CUBE, 32, 4)
    r1 = other(j2, 1)
    rows, res = kernel(residual_kernel, (SD((256, ST), F32), SD((2, 2, SI, BL), F32)), 9, spread, big, 24)(
        j2, r1, r2, r3, tmap, cnt2, ants, m, v)
    zrows = kernel(unpack_kernel, SD((256, ST), F32), 1)(z)
    shape = gains_init.shape
    return rows.reshape(shape), zrows.reshape(shape), res.transpose(0, 2, 1, 3)[None, :, None]


def solution(mesh):
    split = Mesh(mesh.devices.reshape(4, 4, 4, 4, 2), ("x", "y", "zh", "zl", "c"))
    return jax.shard_map(
        on_device,
        mesh=split,
        in_specs=(
            P("x", None, CHAN, None, None, None),
            P("x", None, None, CHAN, None, None, None),
            P("x", CHAN, None, None, None),
            P("x", None, None),
            P(),
            P("x", None, None, CHAN, None, None),
        ),
        out_specs=(
            P("x", None, None, CHAN, None, None),
            P("x", None, None, CHAN, None, None),
            P("x", None, CHAN, None, None, None),
        ),
        check_vma=False,
    )
```

```python
import functools

import jax
import jax.numpy as jnp
import numpy as np
from jax import lax
from jax.experimental import pallas as pl
from jax.experimental.pallas import tpu as pltpu
from jax.sharding import Mesh, PartitionSpec as P

K, SI, ST, BL, CL, CH = 8, 16, 64, 2048, 4, 128
RHO = 128.0
F32, BF16 = jnp.float32, jnp.bfloat16
NT = (((1,), (1,)), ((), ()))
BC = 512
VM = pl.BlockSpec(memory_space=pltpu.VMEM)
SD = jax.ShapeDtypeStruct
CUBE = ("y", "c", "zl")
PLANE = ("y", "c")
CHAN = ("y", "zh", "zl", "c")


def inverse_gram():
    f = np.arange(CH, dtype=np.float64)
    x = (2 * f + 1) / CH - 1
    basis = np.stack([np.ones_like(x), x, 1.5 * x * x - 0.5], axis=1)
    return np.linalg.inv(basis.T @ basis)


GINV = inverse_gram()


def iota(shape, dim):
    return lax.broadcasted_iota(jnp.int32, shape, dim)


def position(y, z, c):
    return (2 * (y * 32 + z * 2 + c) + 1).astype(F32) * (1.0 / CH) - 1.0


def basis_value(n, x):
    return jnp.where(n == 0, 1.0, jnp.where(n == 1, x, jnp.where(n == 2, 1.5 * x * x - 0.5, 0.0)))


def weight_value(n, x):
    second = 1.5 * x * x - 0.5
    rows = [float(g[0]) + float(g[1]) * x + float(g[2]) * second for g in GINV]
    return jnp.where(n == 0, rows[0], jnp.where(n == 1, rows[1], jnp.where(n == 2, rows[2], 0.0)))


def cube_entry(value, j, q):
    x = position(q >> 5, lax.axis_index("zh") * 4 + ((q >> 2) & 3), (q >> 4) & 1)
    return jnp.where((j & 3) == (q & 3), value(j >> 2, x), 0.0)


def cube_down():
    return cube_entry(weight_value, iota((16, 128), 0), iota((16, 128), 1))


def plane_down():
    j, q = iota((48, 128), 0), iota((48, 128), 1)
    zl = (j * 43) >> 9
    j = j - zl * 12
    z = lax.axis_index("zh") * 4 + lax.axis_index("zl")
    same = ((j & 3) == (q & 3)) & (zl == ((q >> 2) & 3))
    return jnp.where(same, weight_value(j >> 2, position(q >> 5, z, (q >> 4) & 1)), 0.0)


def split3(x):
    hi=x.astype(BF16); r=x-hi.astype(F32); mid=r.astype(BF16); lo=(r-mid.astype(F32)).astype(BF16)
    return hi,mid,lo


def split2(x):
    hi=x.astype(BF16)
    return hi,(x-hi.astype(F32)).astype(BF16)


def onehot(ants, side, off):
    ids=ants[side:side+1, pl.ds(off,BC)]
    io=lax.broadcasted_iota(jnp.int32,(ST,BC),0)
    return jnp.where(io==ids,1.0,0.0).astype(BF16)


def gather(g3, oh, out):
    out[...]=jnp.dot(g3, jnp.concatenate([oh,oh,oh],0), preferred_element_type=F32)


def totals_body(gains, ants, m_ref, v_ref, ga2, gc2, x2, acc, low=0, high=BL//BC):
    g3=jnp.concatenate(split3(gains),1)
    if low==0:
        acc[...]=jnp.zeros_like(acc)
    def chunk(c):
        off=c*BC; ga=ga2.at[c%2]; gc=gc2.at[c%2]; x_ref=x2.at[c%2]
        oa=onehot(ants,0,off); oc=onehot(ants,1,off)
        if c==low:
            gather(g3,oa,ga); gather(g3,oc,gc)
        if c+1<high:
            gather(g3,onehot(ants,0,off+BC),ga2.at[(c+1)%2]); gather(g3,onehot(ants,1,off+BC),gc2.at[(c+1)%2])
        for lt in range(BC//128):
            L=slice(lt*128,lt*128+128)
            D=slice(off+lt*128,off+lt*128+128)
            res=[[v_ref[r,t,:,D] for r in range(2)] for t in range(2)]
            for k in range(K):
                ra=slice(k*16,k*16+16); ia=slice(128+k*16,128+k*16+16)
                ar,ai,cr,ci=ga[ra,L],ga[ia,L],gc[ra,L],gc[ia,L]
                pr=ar*cr+ai*ci; pi=ai*cr-ar*ci
                for t in range(2):
                    mr=m_ref[0,t,k,:,D].astype(F32); mi=m_ref[1,t,k,:,D].astype(F32)
                    res[t][0]=res[t][0]-(pr*mr-pi*mi)
                    res[t][1]=res[t][1]-(pr*mi+pi*mr)
            for k in range(K):
                ra=slice(k*16,k*16+16); ia=slice(128+k*16,128+k*16+16)
                ar,ai,cr,ci=ga[ra,L],ga[ia,L],gc[ra,L],gc[ia,L]
                dd=0.0; qr=0.0; qi=0.0
                for t in range(2):
                    mr=m_ref[0,t,k,:,D].astype(F32); mi=m_ref[1,t,k,:,D].astype(F32)
                    rr,ri=res[t]
                    qr=qr+(rr*mr+ri*mi); qi=qi+(ri*mr-rr*mi)
                    dd=dd+(mr*mr+mi*mi)
                vals=((qr*cr-qi*ci, qr*ci+qi*cr, (cr*cr+ci*ci)*dd),
                      (qr*ar+qi*ai, qr*ai-qi*ar, (ar*ar+ai*ai)*dd))
                for s in range(2):
                    LL=slice(s*BC+lt*128,s*BC+lt*128+128)
                    for q in range(3):
                        h,l=split2(vals[s][q])
                        x_ref[q*128+k*16:q*128+k*16+16,LL]=h
                        x_ref[384+q*128+k*16:384+q*128+k*16+16,LL]=l
        oh2=jnp.concatenate([oa,oc],1)
        t=lax.dot_general(x_ref[...],oh2,NT,preferred_element_type=F32)
        acc[...]+=t[:384]+t[384:]
        return 0
    for c in range(low,high): chunk(c)
    if high<BL//BC:
        return
    den=acc[256:384,:]
    acc[0:256,:]=acc[0:256,:]+gains*jnp.concatenate([den,den],0)


def unpack(jp):
    return jnp.concatenate([jp[:, :ST], jp[:, ST:]], 0)


def pack(top, bottom):
    return jnp.concatenate([top, bottom], 1)


def pack_kernel(g_ref, out):
    out[...] = pack(g_ref[0:128, :], g_ref[128:256, :])


def merge(out, fit, tmp, ab):
    tmp[...] = fit
    for r in range(4):
        at = pl.ds(r, 32, stride=4)
        out[pl.ds(r, 32, stride=10), :] = tmp[at, :]
        out[pl.ds(4 + r, 32, stride=10), :] = ab[at, :]
    left = iota((32, 128), 1) < ST
    for p in range(2):
        out[pl.ds(8 + p, 32, stride=10), :] = jnp.where(
            left, ab[pl.ds(128 + 2 * p, 32, stride=4), :], ab[pl.ds(129 + 2 * p, 32, stride=4), :])


def copies(out, value, times):
    rows = value.shape[0]
    for i in range(times):
        out[i * rows:i * rows + rows, :] = value


def early_kernel(g_ref, ants, m_ref, v_ref, sums, ga, gc, x_ref):
    totals_body(g_ref[...], ants, m_ref, v_ref, ga, gc, x_ref, sums, 0, 1)


def first_kernel(g_ref, ants, m_ref, v_ref, sums, ab, ga, gc, x_ref, acc):
    acc[...] = sums[...]
    totals_body(g_ref[...], ants, m_ref, v_ref, ga, gc, x_ref, acc, 1)
    inv = 1.0 / (acc[256:384, :] + RHO)
    inv = pack(inv, inv)
    ab[0:128, :] = pack(acc[0:128, :], acc[128:256, :]) * inv
    ab[128:256, :] = RHO * inv


def mm(a, b):
    a0, a1, a2 = split3(a)
    b0, b1, b2 = split3(b)
    return jnp.dot(jnp.concatenate([a0, a0, a0, a1, a1, a2], 1), jnp.concatenate([b0, b1, b2, b0, b1, b0], 0),
                   preferred_element_type=F32)


def expand(coef):
    j, q = iota((128, 96), 1), iota((128, 96), 0)
    piece = j >> 4
    whole = cube_entry(basis_value, j & 15, q)
    high = whole.astype(BF16).astype(F32)
    rest = whole - high
    middle = rest.astype(BF16).astype(F32)
    up = jnp.where(piece < 3, high, jnp.where(piece < 5, middle, rest - middle)).astype(BF16)
    c0, c1, c2 = split3(coef)
    return jnp.dot(up, jnp.concatenate([c0, c1, c2, c0, c1, c0], 0), preferred_element_type=F32)


def plane_kernel(recv, out):
    copies(out, mm(plane_down(), recv[...]), 4)


def summed(recv, first, count):
    total = recv[first * 12:first * 12 + 12, :]
    for i in range(1, count):
        s = (first + i) * 12
        total = total + recv[s:s + 12, :]
    return jnp.concatenate([total, jnp.zeros((4, 128), F32)], 0)


def fit_kernel(count, recv, ab, out, zh, tmp):
    z = expand(summed(recv, 0, count))
    zh[...] = z
    merge(out, z, tmp, ab)


def coefficients(recv, t_ref, cnt):
    return averaged([summed(recv, h * 4, 4) for h in range(CL)], range(CL), t_ref, cnt)


def last_fit_kernel(recv, t_ref, cnt, out):
    out[...] = expand(coefficients(recv, t_ref, cnt))


def stepped(got, zh, ab, tmp, j_out):
    left = iota((32, 128), 1) < ST
    for r in range(4):
        at = pl.ds(r, 32, stride=4)
        two = got[pl.ds(8 + r // 2, 32, stride=10), :]
        turned = jnp.concatenate([two[:, ST:], two[:, :ST]], 1)
        slope = jnp.where(left, two, turned) if r % 2 == 0 else jnp.where(left, turned, two)
        tmp[at, :] = got[pl.ds(4 + r, 32, stride=10), :] + slope * zh[at, :]
        j_out[at, :] = ab[at, :] + ab[pl.ds(128 + r, 32, stride=4), :] * got[pl.ds(r, 32, stride=10), :]
    return mm(cube_down(), tmp[...])


def update_kernel(got, zh, ab, out, tmp, own):
    part = stepped(got, zh, ab, tmp, own)
    for h in range(CL):
        out[h * 144:h * 144 + 128, :] = own[...]
        out[h * 144 + 128:h * 144 + 144, :] = part


def second_update_kernel(got, zh, ab, part, j_out, tmp):
    copies(part, stepped(got, zh, ab, tmp, j_out)[0:12], 16)


def meet_kernel(recv, t_ref, cnt, out):
    copies(out, averaged([recv[h * 144 + 128:h * 144 + 144, :] for h in range(CL)], range(CL), t_ref, cnt)[0:12], 4)


def map_kernel(mine, theirs, own, ants, t_ref, cnt, kept):
    kept[...] = ants[...]
    shared = mine.shape[1]
    io = lax.broadcasted_iota(jnp.int32, (ST, shared), 0)
    eye = jnp.where(lax.broadcasted_iota(jnp.int32, (ST, ST), 0) == lax.broadcasted_iota(jnp.int32, (ST, ST), 1), 1.0, 0.0)
    zero = jnp.zeros((ST, ST), F32)
    total = jnp.zeros((8, ST), F32)
    ones = jnp.ones((8, shared), BF16)
    for h in range(CL):
        om = jnp.where(io == mine[h:h + 1, :], 1.0, 0.0).astype(BF16)
        ot = jnp.where(io == theirs[h:h + 1, :], 1.0, 0.0).astype(BF16)
        t = lax.dot_general(ot, om, NT, preferred_element_type=F32) + eye * own[h:h + 1, :]
        t_ref[h * 128:h * 128 + 128, :] = pack(jnp.concatenate([t, zero], 0), jnp.concatenate([zero, t], 0)).astype(BF16)
        total = total + lax.dot_general(ones, om, NT, preferred_element_type=F32)
    cnt[...] = 1.0 / (1.0 + pack(total, total))


def averaged(parts, clusters, t_ref, cnt):
    total = 0.0
    for x, h in zip(parts, clusters):
        t = t_ref[pl.ds(pl.multiple_of(h * 128, 128), 128), :]
        total = total + jnp.dot(jnp.concatenate(split3(x), 1), jnp.concatenate([t, t, t], 0), preferred_element_type=F32)
    return total * cnt[0:1, :]


def average_of(own, r1, r2, r3, t_ref, cnt):
    g = lax.axis_index("x")
    return averaged([own[...], r1[...], r2[...], r3[...]], [lax.rem(g + CL - s, CL) for s in range(CL)], t_ref, cnt)


def second_kernel(recv, t_ref, cnt, ants, m_ref, v_ref, ab, ga, gc, x_ref, acc):
    j1 = averaged([recv[h * 144:h * 144 + 128, :] for h in range(CL)], range(CL), t_ref, cnt)
    totals_body(unpack(j1), ants, m_ref, v_ref, ga, gc, x_ref, acc)
    inv = 1.0 / (acc[256:384, :] + RHO)
    inv = pack(inv, inv)
    ab[0:128, :] = (pack(acc[0:128, :], acc[128:256, :]) - RHO * j1) * inv
    ab[128:256, :] = (2.0 * RHO) * inv


def gate_kernel(x_ref, out):
    out[...] = x_ref[...]


def unpack_kernel(z_ref, out):
    out[...] = unpack(z_ref[...])


def residual_kernel(own, r1, r2, r3, t_ref, cnt, ants, m_ref, v_ref, rows, out, ga, gc):
    gains = unpack(average_of(own, r1, r2, r3, t_ref, cnt))
    rows[...] = gains
    g3 = jnp.concatenate(split3(gains), 1)
    def chunk(c,_):
        off=pl.multiple_of(c*BC,BC)
        gather(g3,onehot(ants,0,off),ga); gather(g3,onehot(ants,1,off),gc)
        for lt in range(BC//128):
            L=slice(lt*128,lt*128+128)
            D=pl.ds(pl.multiple_of(off+lt*128,128),128)
            res=[[v_ref[r,t,:,D] for r in range(2)] for t in range(2)]
            for k in range(K):
                ra=slice(k*16,k*16+16); ia=slice(128+k*16,128+k*16+16)
                ar,ai,cr,ci=ga[ra,L],ga[ia,L],gc[ra,L],gc[ia,L]
                pr=ar*cr+ai*ci; pi=ai*cr-ar*ci
                for t in range(2):
                    mr=m_ref[0,t,k,:,D].astype(F32); mi=m_ref[1,t,k,:,D].astype(F32)
                    res[t][0]=res[t][0]-(pr*mr-pi*mi)
                    res[t][1]=res[t][1]-(pr*mi+pi*mr)
            for t in range(2):
                for r in range(2): out[r,t,:,D]=res[t][r]
        return 0
    lax.fori_loop(0,BL//BC,chunk,0,unroll=4)


def kernel(body, outs, ins, scratch=(), flops=100000000, vmem=8, moved=1000000):
    return pl.pallas_call(
        body, out_shape=outs, in_specs=[VM] * ins,
        out_specs=(VM,) * len(outs) if isinstance(outs, tuple) else VM,
        scratch_shapes=list(scratch),
        compiler_params=pltpu.CompilerParams(vmem_limit_bytes=vmem * 1048576),
        cost_estimate=pl.CostEstimate(flops=flops, bytes_accessed=moved, transcendentals=0))


def on_device(visibilities, model, flags, antennas, correlation, gains_init):
    ants = antennas[0]
    gains = gains_init.reshape(2 * K * SI, ST)
    group = lax.axis_index("x")
    mine = lax.dynamic_index_in_dim(correlation, group, 0, keepdims=False)
    theirs = lax.dynamic_index_in_dim(correlation, group, 1, keepdims=False)
    own = jnp.broadcast_to(jnp.where(jnp.arange(CL) == group, 1.0, 0.0)[:, None], (CL, ST))
    full = SD((128, 128), F32)
    tile = pltpu.VMEM((128, 128), F32)
    exchange = functools.partial(lax.all_to_all, split_axis=0, concat_axis=0, tiled=True)
    scratch = [pltpu.VMEM((2, 256, BC), F32), pltpu.VMEM((2, 256, BC), F32), pltpu.VMEM((2, 768, 2 * BC), BF16), pltpu.VMEM((384, ST), F32)]
    spread = [pltpu.VMEM((256, BC), F32), pltpu.VMEM((256, BC), F32)]
    big = 2000000000
    wide = SD((320, 128), F32)
    pairs = SD((256, 128), F32)
    moments = SD((192, 128), F32)

    def others(j):
        return [lax.ppermute(j, "x", [(i, (i + s) % CL) for i in range(CL)]) for s in range(1, CL)]

    def swap(x, axes, *shape):
        return exchange(x.reshape(*shape, 128), axes).reshape(-1, 128)

    got = swap(kernel(pack_kernel, full, 1, flops=20000000000, moved=20000000)(gains), PLANE, 8, 16)
    keep = flags[0, 0] == 0
    m = jnp.where(keep[None, None], model[0][:, :, 0], jnp.zeros((), BF16)).transpose(0, 3, 1, 2, 4)
    v = jnp.where(keep[None], visibilities[0][:, 0], 0.0).transpose(0, 2, 1, 3)
    tmap, cnt, ants = kernel(map_kernel, (SD((CL * 128, 128), BF16), SD((8, 128), F32), SD((2, BL), jnp.int32)), 4)(
        mine, theirs, own, ants)
    sums = kernel(early_kernel, SD((384, ST), F32), 4, scratch[:3], big // 4, 24)(gains, ants, m, v)
    got, m, v, tmap, cnt, ants, sums = lax.optimization_barrier((got, m, v, tmap, cnt, ants, sums))
    got = swap(kernel(plane_kernel, moments, 1)(got), ("zh", "zl"), 16, 3, 4)
    ab = kernel(first_kernel, pairs, 5, scratch, big, 24)(gains, ants, m, v, sums)

    got, ab = lax.optimization_barrier((got, ab))
    send, zh = kernel(functools.partial(fit_kernel, 16), (wide, full), 2, [tile])(got, ab)
    got = swap(send, CUBE, 32, 5, 2)
    recv = exchange(kernel(update_kernel, SD((576, 128), F32), 3, [tile, tile])(got, zh, ab), "x")
    part = kernel(meet_kernel, SD((48, 128), F32), 3)(recv, tmap, cnt)
    got = swap(part, "zh", 4, 3, 4)
    ab = kernel(second_kernel, pairs, 6, scratch, big, 24)(recv, tmap, cnt, ants, m, v)
    send, zh = kernel(functools.partial(fit_kernel, 4), (wide, full), 2, [tile])(got, ab)
    got = swap(send, CUBE, 32, 5, 2)
    part, j2 = kernel(second_update_kernel, (moments, full), 3, [tile])(got, zh, ab)
    got = swap(part, ("x", "zh"), 16, 3, 4)
    d2 = others(j2)
    cnt2 = kernel(gate_kernel, SD((8, 128), F32), 1)(cnt)
    rows, res = kernel(residual_kernel, (SD((256, ST), F32), SD((2, 2, SI, BL), F32)), 9, spread, big, 24)(
        j2, *d2, tmap, cnt2, ants, m, v)
    z = kernel(last_fit_kernel, full, 3)(got, tmap, cnt)
    zrows = kernel(unpack_kernel, SD((256, ST), F32), 1)(swap(z, CUBE, 32, 4))
    shape = gains_init.shape
    return rows.reshape(shape), zrows.reshape(shape), res.transpose(0, 2, 1, 3)[None, :, None]


def solution(mesh):
    split = Mesh(mesh.devices.reshape(4, 4, 4, 4, 2), ("x", "y", "zh", "zl", "c"))
    return jax.shard_map(
        on_device,
        mesh=split,
        in_specs=(
            P("x", None, CHAN, None, None, None),
            P("x", None, None, CHAN, None, None, None),
            P("x", CHAN, None, None, None),
            P("x", None, None),
            P(),
            P("x", None, None, CHAN, None, None),
        ),
        out_specs=(
            P("x", None, None, CHAN, None, None),
            P("x", None, None, CHAN, None, None),
            P("x", None, CHAN, None, None, None),
        ),
        check_vma=False,
    )
```

```python
import functools

import jax
import jax.numpy as jnp
import numpy as np
from jax import lax
from jax.experimental import pallas as pl
from jax.experimental.pallas import tpu as pltpu
from jax.sharding import Mesh, PartitionSpec as P

K, SI, ST, BL, CL, CH = 8, 16, 64, 2048, 4, 128
RHO = 128.0
F32, BF16 = jnp.float32, jnp.bfloat16
NT = (((1,), (1,)), ((), ()))
BC = 1024
VM = pl.BlockSpec(memory_space=pltpu.VMEM)
SD = jax.ShapeDtypeStruct
CUBE = ("y", "c", "zl")
PLANE = ("y", "c")
CHAN = ("y", "zh", "zl", "c")


def inverse_gram():
    f = np.arange(CH, dtype=np.float64)
    x = (2 * f + 1) / CH - 1
    basis = np.stack([np.ones_like(x), x, 1.5 * x * x - 0.5], axis=1)
    return np.linalg.inv(basis.T @ basis)


GINV = inverse_gram()


def iota(shape, dim):
    return lax.broadcasted_iota(jnp.int32, shape, dim)


def position(y, z, c):
    return (2 * (y * 32 + z * 2 + c) + 1).astype(F32) * (1.0 / CH) - 1.0


def basis_value(n, x):
    return jnp.where(n == 0, 1.0, jnp.where(n == 1, x, jnp.where(n == 2, 1.5 * x * x - 0.5, 0.0)))


def weight_value(n, x):
    second = 1.5 * x * x - 0.5
    rows = [float(g[0]) + float(g[1]) * x + float(g[2]) * second for g in GINV]
    return jnp.where(n == 0, rows[0], jnp.where(n == 1, rows[1], jnp.where(n == 2, rows[2], 0.0)))


def cube_entry(value, j, q):
    x = position(q >> 5, lax.axis_index("zh") * 4 + ((q >> 2) & 3), (q >> 4) & 1)
    return jnp.where((j & 3) == (q & 3), value(j >> 2, x), 0.0)


def cube_down():
    return cube_entry(weight_value, iota((16, 128), 0), iota((16, 128), 1))


def plane_down():
    j, q = iota((48, 128), 0), iota((48, 128), 1)
    zl = (j * 43) >> 9
    j = j - zl * 12
    z = lax.axis_index("zh") * 4 + lax.axis_index("zl")
    same = ((j & 3) == (q & 3)) & (zl == ((q >> 2) & 3))
    return jnp.where(same, weight_value(j >> 2, position(q >> 5, z, (q >> 4) & 1)), 0.0)


def split3(x):
    hi=x.astype(BF16); r=x-hi.astype(F32); mid=r.astype(BF16); lo=(r-mid.astype(F32)).astype(BF16)
    return hi,mid,lo


def split2(x):
    hi=x.astype(BF16)
    return hi,(x-hi.astype(F32)).astype(BF16)


def onehot(ants, side, off):
    ids=ants[side:side+1, pl.ds(off,BC)]
    io=lax.broadcasted_iota(jnp.int32,(ST,BC),0)
    return jnp.where(io==ids,1.0,0.0).astype(BF16)


def gather(g3, oh, out):
    out[...]=jnp.dot(g3, jnp.concatenate([oh,oh,oh],0), preferred_element_type=F32)


def totals_body(gains, ants, m_ref, v_ref, ga2, gc2, x2, acc):
    g3=jnp.concatenate(split3(gains),1)
    acc[...]=jnp.zeros_like(acc)
    def chunk(c):
        off=c*BC; ga=ga2.at[c%2]; gc=gc2.at[c%2]; x_ref=x2.at[c%2]
        oa=onehot(ants,0,off); oc=onehot(ants,1,off)
        if c==0:
            gather(g3,oa,ga); gather(g3,oc,gc)
        if c+1<BL//BC:
            gather(g3,onehot(ants,0,off+BC),ga2.at[(c+1)%2]); gather(g3,onehot(ants,1,off+BC),gc2.at[(c+1)%2])
        for lt in range(BC//128):
            L=slice(lt*128,lt*128+128)
            D=slice(off+lt*128,off+lt*128+128)
            res=[[v_ref[r,t,:,D] for r in range(2)] for t in range(2)]
            for k in range(K):
                ra=slice(k*16,k*16+16); ia=slice(128+k*16,128+k*16+16)
                ar,ai,cr,ci=ga[ra,L],ga[ia,L],gc[ra,L],gc[ia,L]
                pr=ar*cr+ai*ci; pi=ai*cr-ar*ci
                for t in range(2):
                    mr=m_ref[0,t,k,:,D].astype(F32); mi=m_ref[1,t,k,:,D].astype(F32)
                    res[t][0]=res[t][0]-(pr*mr-pi*mi)
                    res[t][1]=res[t][1]-(pr*mi+pi*mr)
            for k in range(K):
                ra=slice(k*16,k*16+16); ia=slice(128+k*16,128+k*16+16)
                ar,ai,cr,ci=ga[ra,L],ga[ia,L],gc[ra,L],gc[ia,L]
                dd=0.0; qr=0.0; qi=0.0
                for t in range(2):
                    mr=m_ref[0,t,k,:,D].astype(F32); mi=m_ref[1,t,k,:,D].astype(F32)
                    rr,ri=res[t]
                    qr=qr+(rr*mr+ri*mi); qi=qi+(ri*mr-rr*mi)
                    dd=dd+(mr*mr+mi*mi)
                vals=((qr*cr-qi*ci, qr*ci+qi*cr, (cr*cr+ci*ci)*dd),
                      (qr*ar+qi*ai, qr*ai-qi*ar, (ar*ar+ai*ai)*dd))
                for s in range(2):
                    LL=slice(s*BC+lt*128,s*BC+lt*128+128)
                    for q in range(3):
                        h,l=split2(vals[s][q])
                        x_ref[q*128+k*16:q*128+k*16+16,LL]=h
                        x_ref[384+q*128+k*16:384+q*128+k*16+16,LL]=l
        oh2=jnp.concatenate([oa,oc],1)
        t=lax.dot_general(x_ref[...],oh2,NT,preferred_element_type=F32)
        acc[...]+=t[:384]+t[384:]
        return 0
    for c in range(BL//BC): chunk(c)
    den=acc[256:384,:]
    acc[0:256,:]=acc[0:256,:]+gains*jnp.concatenate([den,den],0)


def unpack(jp):
    return jnp.concatenate([jp[:, :ST], jp[:, ST:]], 0)


def pack(top, bottom):
    return jnp.concatenate([top, bottom], 1)


def pack_kernel(g_ref, out):
    out[...] = pack(g_ref[0:128, :], g_ref[128:256, :])


def merge(out, fit, tmp, ab):
    tmp[...] = fit
    for r in range(4):
        at = pl.ds(r, 32, stride=4)
        out[pl.ds(r, 32, stride=10), :] = tmp[at, :]
        out[pl.ds(4 + r, 32, stride=10), :] = ab[at, :]
    left = iota((32, 128), 1) < ST
    for p in range(2):
        out[pl.ds(8 + p, 32, stride=10), :] = jnp.where(
            left, ab[pl.ds(128 + 2 * p, 32, stride=4), :], ab[pl.ds(129 + 2 * p, 32, stride=4), :])


def copies(out, value, times):
    rows = value.shape[0]
    for i in range(times):
        out[i * rows:i * rows + rows, :] = value


def first_kernel(g_ref, ants, m_ref, v_ref, ab, ga, gc, x_ref, acc):
    totals_body(g_ref[...], ants, m_ref, v_ref, ga, gc, x_ref, acc)
    inv = 1.0 / (acc[256:384, :] + RHO)
    inv = pack(inv, inv)
    ab[0:128, :] = pack(acc[0:128, :], acc[128:256, :]) * inv
    ab[128:256, :] = RHO * inv


def mm(a, b):
    a0, a1, a2 = split3(a)
    b0, b1, b2 = split3(b)
    return jnp.dot(jnp.concatenate([a0, a0, a0, a1, a1, a2], 1), jnp.concatenate([b0, b1, b2, b0, b1, b0], 0),
                   preferred_element_type=F32)


def expand(coef):
    j, q = iota((128, 96), 1), iota((128, 96), 0)
    piece = j >> 4
    whole = cube_entry(basis_value, j & 15, q)
    high = whole.astype(BF16).astype(F32)
    rest = whole - high
    middle = rest.astype(BF16).astype(F32)
    up = jnp.where(piece < 3, high, jnp.where(piece < 5, middle, rest - middle)).astype(BF16)
    c0, c1, c2 = split3(coef)
    return jnp.dot(up, jnp.concatenate([c0, c1, c2, c0, c1, c0], 0), preferred_element_type=F32)


def plane_kernel(recv, out):
    copies(out, mm(plane_down(), recv[...]), 4)


def summed(recv, first, count):
    total = recv[first * 12:first * 12 + 12, :]
    for i in range(1, count):
        s = (first + i) * 12
        total = total + recv[s:s + 12, :]
    return jnp.concatenate([total, jnp.zeros((4, 128), F32)], 0)


def fit_kernel(count, recv, ab, out, zh, tmp):
    z = expand(summed(recv, 0, count))
    zh[...] = z
    merge(out, z, tmp, ab)


def coefficients(recv, t_ref, cnt):
    return averaged([summed(recv, h * 4, 4) for h in range(CL)], range(CL), t_ref, cnt)


def last_fit_kernel(recv, t_ref, cnt, out):
    out[...] = expand(coefficients(recv, t_ref, cnt))


def stepped(got, zh, ab, tmp, j_out):
    left = iota((32, 128), 1) < ST
    for r in range(4):
        at = pl.ds(r, 32, stride=4)
        two = got[pl.ds(8 + r // 2, 32, stride=10), :]
        turned = jnp.concatenate([two[:, ST:], two[:, :ST]], 1)
        slope = jnp.where(left, two, turned) if r % 2 == 0 else jnp.where(left, turned, two)
        tmp[at, :] = got[pl.ds(4 + r, 32, stride=10), :] + slope * zh[at, :]
        j_out[at, :] = ab[at, :] + ab[pl.ds(128 + r, 32, stride=4), :] * got[pl.ds(r, 32, stride=10), :]
    return mm(cube_down(), tmp[...])


def update_kernel(got, zh, ab, out, tmp, own):
    part = stepped(got, zh, ab, tmp, own)
    for h in range(CL):
        out[h * 144:h * 144 + 128, :] = own[...]
        out[h * 144 + 128:h * 144 + 144, :] = part


def second_update_kernel(got, zh, ab, part, j_out, tmp):
    copies(part, stepped(got, zh, ab, tmp, j_out)[0:12], 16)


def meet_kernel(recv, t_ref, cnt, out):
    copies(out, averaged([recv[h * 144 + 128:h * 144 + 144, :] for h in range(CL)], range(CL), t_ref, cnt)[0:12], 4)


def map_kernel(mine, theirs, own, ants, t_ref, cnt, kept):
    kept[...] = ants[...]
    shared = mine.shape[1]
    io = lax.broadcasted_iota(jnp.int32, (ST, shared), 0)
    eye = jnp.where(lax.broadcasted_iota(jnp.int32, (ST, ST), 0) == lax.broadcasted_iota(jnp.int32, (ST, ST), 1), 1.0, 0.0)
    zero = jnp.zeros((ST, ST), F32)
    total = jnp.zeros((8, ST), F32)
    ones = jnp.ones((8, shared), BF16)
    for h in range(CL):
        om = jnp.where(io == mine[h:h + 1, :], 1.0, 0.0).astype(BF16)
        ot = jnp.where(io == theirs[h:h + 1, :], 1.0, 0.0).astype(BF16)
        t = lax.dot_general(ot, om, NT, preferred_element_type=F32) + eye * own[h:h + 1, :]
        t_ref[h * 128:h * 128 + 128, :] = pack(jnp.concatenate([t, zero], 0), jnp.concatenate([zero, t], 0)).astype(BF16)
        total = total + lax.dot_general(ones, om, NT, preferred_element_type=F32)
    cnt[...] = 1.0 / (1.0 + pack(total, total))


def averaged(parts, clusters, t_ref, cnt):
    total = 0.0
    for x, h in zip(parts, clusters):
        t = t_ref[pl.ds(pl.multiple_of(h * 128, 128), 128), :]
        total = total + jnp.dot(jnp.concatenate(split3(x), 1), jnp.concatenate([t, t, t], 0), preferred_element_type=F32)
    return total * cnt[0:1, :]


def average_of(own, r1, r2, r3, t_ref, cnt):
    g = lax.axis_index("x")
    return averaged([own[...], r1[...], r2[...], r3[...]], [lax.rem(g + CL - s, CL) for s in range(CL)], t_ref, cnt)


def second_kernel(recv, t_ref, cnt, ants, m_ref, v_ref, ab, ga, gc, x_ref, acc):
    j1 = averaged([recv[h * 144:h * 144 + 128, :] for h in range(CL)], range(CL), t_ref, cnt)
    totals_body(unpack(j1), ants, m_ref, v_ref, ga, gc, x_ref, acc)
    inv = 1.0 / (acc[256:384, :] + RHO)
    inv = pack(inv, inv)
    ab[0:128, :] = (pack(acc[0:128, :], acc[128:256, :]) - RHO * j1) * inv
    ab[128:256, :] = (2.0 * RHO) * inv


def gate_kernel(x_ref, out):
    out[...] = x_ref[...]


def unpack_kernel(z_ref, out):
    out[...] = unpack(z_ref[...])


def residual_kernel(own, r1, r2, r3, t_ref, cnt, ants, m_ref, v_ref, rows, out, ga, gc):
    gains = unpack(average_of(own, r1, r2, r3, t_ref, cnt))
    rows[...] = gains
    g3 = jnp.concatenate(split3(gains), 1)
    def chunk(c,_):
        off=pl.multiple_of(c*BC,BC)
        gather(g3,onehot(ants,0,off),ga); gather(g3,onehot(ants,1,off),gc)
        for lt in range(BC//128):
            L=slice(lt*128,lt*128+128)
            D=pl.ds(pl.multiple_of(off+lt*128,128),128)
            res=[[v_ref[r,t,:,D] for r in range(2)] for t in range(2)]
            for k in range(K):
                ra=slice(k*16,k*16+16); ia=slice(128+k*16,128+k*16+16)
                ar,ai,cr,ci=ga[ra,L],ga[ia,L],gc[ra,L],gc[ia,L]
                pr=ar*cr+ai*ci; pi=ai*cr-ar*ci
                for t in range(2):
                    mr=m_ref[0,t,k,:,D].astype(F32); mi=m_ref[1,t,k,:,D].astype(F32)
                    res[t][0]=res[t][0]-(pr*mr-pi*mi)
                    res[t][1]=res[t][1]-(pr*mi+pi*mr)
            for t in range(2):
                for r in range(2): out[r,t,:,D]=res[t][r]
        return 0
    lax.fori_loop(0,BL//BC,chunk,0,unroll=2)


def kernel(body, outs, ins, scratch=(), flops=100000000, vmem=8, moved=1000000):
    return pl.pallas_call(
        body, out_shape=outs, in_specs=[VM] * ins,
        out_specs=(VM,) * len(outs) if isinstance(outs, tuple) else VM,
        scratch_shapes=list(scratch),
        compiler_params=pltpu.CompilerParams(vmem_limit_bytes=vmem * 1048576),
        cost_estimate=pl.CostEstimate(flops=flops, bytes_accessed=moved, transcendentals=0))


def on_device(visibilities, model, flags, antennas, correlation, gains_init):
    ants = antennas[0]
    gains = gains_init.reshape(2 * K * SI, ST)
    group = lax.axis_index("x")
    mine = lax.dynamic_index_in_dim(correlation, group, 0, keepdims=False)
    theirs = lax.dynamic_index_in_dim(correlation, group, 1, keepdims=False)
    own = jnp.broadcast_to(jnp.where(jnp.arange(CL) == group, 1.0, 0.0)[:, None], (CL, ST))
    full = SD((128, 128), F32)
    tile = pltpu.VMEM((128, 128), F32)
    exchange = functools.partial(lax.all_to_all, split_axis=0, concat_axis=0, tiled=True)
    scratch = [pltpu.VMEM((2, 256, BC), F32), pltpu.VMEM((2, 256, BC), F32), pltpu.VMEM((2, 768, 2 * BC), BF16), pltpu.VMEM((384, ST), F32)]
    spread = [pltpu.VMEM((256, BC), F32), pltpu.VMEM((256, BC), F32)]
    big = 2000000000
    wide = SD((320, 128), F32)
    pairs = SD((256, 128), F32)
    moments = SD((192, 128), F32)

    def others(j):
        return [lax.ppermute(j, "x", [(i, (i + s) % CL) for i in range(CL)]) for s in range(1, CL)]

    def swap(x, axes, *shape):
        return exchange(x.reshape(*shape, 128), axes).reshape(-1, 128)

    got = swap(kernel(pack_kernel, full, 1, flops=20000000000, moved=20000000)(gains), PLANE, 8, 16)
    keep = flags[0, 0] == 0
    m = jnp.where(keep[None, None], model[0][:, :, 0], jnp.zeros((), BF16)).transpose(0, 3, 1, 2, 4)
    v = jnp.where(keep[None], visibilities[0][:, 0], 0.0).transpose(0, 2, 1, 3)
    tmap, cnt, ants = kernel(map_kernel, (SD((CL * 128, 128), BF16), SD((8, 128), F32), SD((2, BL), jnp.int32)), 4)(
        mine, theirs, own, ants)
    got, m, v, tmap, cnt, ants = lax.optimization_barrier((got, m, v, tmap, cnt, ants))
    got = swap(kernel(plane_kernel, moments, 1)(got), ("zh", "zl"), 16, 3, 4)
    ab = kernel(first_kernel, pairs, 4, scratch, big, 24)(gains, ants, m, v)

    got, ab = lax.optimization_barrier((got, ab))
    send, zh = kernel(functools.partial(fit_kernel, 16), (wide, full), 2, [tile])(got, ab)
    got = swap(send, CUBE, 32, 5, 2)
    recv = exchange(kernel(update_kernel, SD((576, 128), F32), 3, [tile, tile])(got, zh, ab), "x")
    part = kernel(meet_kernel, SD((48, 128), F32), 3)(recv, tmap, cnt)
    got = swap(part, "zh", 4, 3, 4)
    ab = kernel(second_kernel, pairs, 6, scratch, big, 24)(recv, tmap, cnt, ants, m, v)
    send, zh = kernel(functools.partial(fit_kernel, 4), (wide, full), 2, [tile])(got, ab)
    got = swap(send, CUBE, 32, 5, 2)
    part, j2 = kernel(second_update_kernel, (moments, full), 3, [tile])(got, zh, ab)
    got = swap(part, ("x", "zh"), 16, 3, 4)
    d2 = others(j2)
    cnt2 = kernel(gate_kernel, SD((8, 128), F32), 1)(cnt)
    rows, res = kernel(residual_kernel, (SD((256, ST), F32), SD((2, 2, SI, BL), F32)), 9, spread, big, 24)(
        j2, *d2, tmap, cnt2, ants, m, v)
    z = kernel(last_fit_kernel, full, 3)(got, tmap, cnt)
    zrows = kernel(unpack_kernel, SD((256, ST), F32), 1)(swap(z, CUBE, 32, 4))
    shape = gains_init.shape
    return rows.reshape(shape), zrows.reshape(shape), res.transpose(0, 2, 1, 3)[None, :, None]


def solution(mesh):
    split = Mesh(mesh.devices.reshape(4, 4, 4, 4, 2), ("x", "y", "zh", "zl", "c"))
    return jax.shard_map(
        on_device,
        mesh=split,
        in_specs=(
            P("x", None, CHAN, None, None, None),
            P("x", None, None, CHAN, None, None, None),
            P("x", CHAN, None, None, None),
            P("x", None, None),
            P(),
            P("x", None, None, CHAN, None, None),
        ),
        out_specs=(
            P("x", None, None, CHAN, None, None),
            P("x", None, None, CHAN, None, None),
            P("x", None, CHAN, None, None, None),
        ),
        check_vma=False,
    )
```
